32 devices in a mesh: dp: 4 (over x, core), tensor: 8 (over z, y).
Axes of the slice: x: 2, y: 2, z: 4, core: 2. Of those that a mesh axis runs over, the one named last changes fastest.
Arguments:
- grad_out: bfloat16 [256, 4096], P(('dp', 'tensor')), may hold values from -6 to 6
- gate_pre: bfloat16 [256, 14848], P('dp', 'tensor'), may hold values from -8 to 8
- up_pre: bfloat16 [256, 14848], P('dp', 'tensor'), may hold values from -6 to 6
- down_weight: bfloat16 [4096, 14848], P(None, 'tensor'), may hold values from -1.5 to 1.5
Outputs:
- grad_weight: float32 [4096, 14848], P('dp', 'tensor')
- grad_gate: bfloat16 [256, 14848], P('dp', 'tensor')
- grad_up: bfloat16 [256, 14848], P('dp', 'tensor')
The draws below stay inside these ranges and needn't reach their ends.
All inputs are finite; a program needn't handle non-finite values.
Results may differ from the reference program's by a relative error of at most 0.015.
Values may be sent and summed in bfloat16 or wider, within the bound.
A program may use at most 128 MiB of HBM per device.

```python
import jax
import jax.numpy as jnp
from jax import lax

D_W = 4096
FF_W = 14848
TOKG = 64
TOKENS = 256
N_DP = 4


def raised(array, key, source, target, blocks, factor):
    def block_of(dim):
        return (jnp.arange(array.shape[dim]) // (array.shape[dim] // blocks)).reshape((-1,) + (1,) * (array.ndim - 1 - dim))

    near = jax.random.permutation(key, blocks)[block_of(target)]
    far = (block_of(target) + blocks // 2) % blocks
    return jnp.where((block_of(source) == near) | (block_of(source) == far), factor * array, array)


def shard_levels(own_key, shape, cuts, low, high):
    def one(dim, parts):
        draws = jax.random.uniform(jax.random.fold_in(jax.random.fold_in(own_key, 6), dim), (parts,), jnp.float32, low / len(cuts), high / len(cuts))
        return jnp.repeat(jnp.exp(draws), shape[dim] // parts).reshape((-1,) + (1,) * (len(shape) - dim - 1))

    loudness = one(*cuts[0])
    for cut in cuts[1:]:
        loudness = loudness * one(*cut)
    return loudness


def normal_values(rng, shape, scale, bound, split=(), held_as=jnp.bfloat16):
    array = jax.random.normal(rng, shape, jnp.float32) * scale
    if len(split) > 0:
        array = shard_levels(rng, shape, split, -0.22, 0.18) * array
    return jnp.clip(array, min=-bound, max=bound).astype(held_as)


def gaussian_with(stream_key, dims, width, most, shards, heavy, kind=jnp.bfloat16):
    values = width * jax.random.normal(stream_key, dims, jnp.float32)
    if shards:
        values = values * shard_levels(stream_key, dims, shards, -0.22, 0.18)
    return jnp.clip(raised(values, jax.random.fold_in(stream_key, 3), *heavy), -most, most).astype(kind)


def setup_inputs(seed: int = 0) -> dict:
    seeds = jax.random.split(jax.random.key(seed), 5)
    grad_out = gaussian_with(seeds[0], (TOKENS, D_W), (4 * TOKENS ** -0.5), 6.0, ((0, 32),), (0, 1, 32, 2.75))
    gate_pre = normal_values(seeds[1], (TOKENS, FF_W), 2.0, 8.0, ((0, 4), (1, 8)))
    up_pre = normal_values(seeds[2], (TOKENS, FF_W), 1.0, 6.0, ((0, 4), (1, 8)))
    down_weight = normal_values(seeds[3], (D_W, FF_W), (max(D_W // 256, 1)) ** -0.5, 1.5, ((1, 8),))
    return dict(grad_out=grad_out, gate_pre=gate_pre, up_pre=up_pre, down_weight=down_weight)


def reference(grad_out, gate_pre, up_pre, down_weight):
    gate = gate_pre.astype(jnp.float32)
    upper = up_pre.astype(jnp.float32)
    sig = jax.nn.sigmoid(gate)
    act = gate * sig
    hidden = (act * upper).astype(jnp.bfloat16)
    grad_hidden = jnp.dot(grad_out, down_weight, preferred_element_type=jnp.float32)
    grad_up = (grad_hidden * act).astype(jnp.bfloat16)
    grad_gate = (grad_hidden * upper * sig * (1.0 + gate * (1.0 - sig))).astype(jnp.bfloat16)
    grouped_out = grad_out.reshape(N_DP, TOKG, D_W)
    grouped_hidden = hidden.reshape(N_DP, TOKG, FF_W)

    def add_group(total, pair):
        part = jnp.dot(pair[0].T, pair[1], preferred_element_type=jnp.float32)
        rounded = lax.optimization_barrier(part.astype(jnp.bfloat16))
        return total + rounded.astype(jnp.float32), None

    grad_weight, unused = lax.scan(add_group, jnp.zeros((D_W, FF_W), jnp.float32), (grouped_out, grouped_hidden))
    return grad_weight, grad_gate, grad_up
```

```python
import functools

import jax
import jax.numpy as jnp
from jax import lax
from jax.experimental import pallas as pl
from jax.experimental.pallas import tpu as pltpu
from jax.sharding import PartitionSpec as P

MESH = pl.DeviceIdType.MESH
CORES = 2
VMEM = 67043328


def cut(wide, step):
    return [(start, min(step, wide - start)) for start in range(0, wide, step)]


def gather_kernel(
    n_dp, n_t, outer, spans, pieces,
    go_hbm, gate_hbm, up_hbm, weight_hbm,
    cols_ref, hidden_ref, grad_ref, other_ref, act_ref, slope_ref,
    mine, extra, gate, upper, weight, left, acc, leave,
    load_sem, weight_sem, send_sem,
    own_sem, extra_sem, cross_sem, cols_sem, far_sem, hidden_sem, pair_sem, grad_sem,
):
    inner = n_t // outer
    n_chip = n_dp // CORES
    depth, feats = mine.shape[0], cols_ref.shape[-1]
    dp, t = lax.axis_index("dp"), lax.axis_index("tensor")
    chip, core = dp // CORES, dp % CORES
    mate = chip * CORES + (1 - core)
    a, b = t // inner, t % inner
    chips = [lax.rem(chip + d, n_chip) for d in range(1, n_chip)]
    sides = [lax.rem(b + d, inner) for d in range(1, inner)]

    has_line = outer == 4
    between = (a * (3 - a)) // 2
    twin, mirror, across = a + 1 - 2 * (a % 2), 3 - a, (a + 2) % 4
    first = between * mirror + (1 - between) * twin
    second = between * twin + (1 - between) * mirror
    line = [first, second, across] if has_line else []

    def at(step, side):
        return step * inner + side

    loads = [
        pltpu.make_async_copy(go_hbm, mine, load_sem.at[0]),
        pltpu.make_async_copy(gate_hbm, gate, load_sem.at[1]),
        pltpu.make_async_copy(up_hbm, upper, load_sem.at[2]),
    ]
    for load in loads:
        load.start()

    barrier = pltpu.get_barrier_semaphore()
    peers = [(lax.rem(dp + d, n_dp), t) for d in range(1, n_dp)]
    for c in range(CORES):
        peers += [(chip * CORES + c, at(step, b)) for step in line]
        peers += [(chip * CORES + c, at(a, side)) for side in sides]
    for peer in peers:
        pl.semaphore_signal(barrier, inc=1, device_id=peer, device_id_type=MESH)
    with jax.named_scope("go"):
        loads[0].wait()
    with jax.named_scope("barrier"):
        pl.semaphore_wait(barrier, len(peers))

    sent = []

    def copy_to(block, sem, peer, dst=None, slot=None):
        copy = pltpu.make_async_remote_copy(
            src_ref=block, dst_ref=block if dst is None else dst,
            send_sem=send_sem.at[len(sent) if slot is None else slot], recv_sem=sem,
            device_id=peer, device_id_type=MESH,
        )
        if slot is None:
            sent.append(copy)
        return copy

    def send(block, sem, peer, dst=None):
        copy_to(block, sem, peer, dst).start()

    def send_two(block, sem, peers, dst=None):
        slot = len(sent)
        for peer in peers:
            copy_to(block, sem, peer, dst, slot).start()
        sent.append(copy_to(cols_ref.at[chip, :, t], sem, peers[0], None, slot))

    def arrived(block, sem):
        pltpu.make_async_remote_copy(
            src_ref=block, dst_ref=block, send_sem=send_sem.at[0], recv_sem=sem,
            device_id=(mate, t), device_id_type=MESH,
        ).wait_recv()

    def block_of(group):
        return pl.ds(pl.multiple_of(group * feats, feats), feats)

    def spread(block, sem, group, dst=None):
        slot = None
        if has_line:
            send_two(block, sem, [(group, at(twin, b)), (group, at(mirror, b))], dst)
            slot = len(sent)
            last = copy_to(block, sem, (group, at(across, b)), dst)

            @pl.when(between == 0)
            def _():
                last.start()
        return slot

    def relay(block, sem, slot):
        @pl.when(between == 1)
        def _():
            copy_to(block, sem, (dp, at(twin, b)), slot=slot).start()

    for other in chips:
        for c in range(CORES):
            group = other * CORES + c
            send(mine.at[:, block_of(group)], cross_sem.at[chip, core], (group, t), cols_ref.at[chip, core, t])

    def own_block(source, dst, sem):
        slots = []
        for c in range(CORES):
            group = chip * CORES + c
            block = mine.at[:, block_of(source * CORES + c)]
            for side in sides:
                send(block, sem, (group, at(a, side)), dst)
            slots.append(spread(block, sem, group, dst))
        send(mine.at[:, block_of(source * CORES + 1 - core)], sem, (mate, t), dst)
        return slots

    own_slots = own_block(chip, cols_ref.at[chip, core, t], own_sem.at[t])
    extra_slots = [own_block(other, extra.at[other, core, t], extra_sem.at[other, core, t]) for other in chips]

    with jax.named_scope("hid_load"):
        loads[1].wait()
        loads[2].wait()
    kinds = [chip] + chips
    weight_loads = [
        [
            pltpu.make_async_copy(
                weight_hbm.at[pl.ds(start, width), block_of(kind * CORES + core)],
                weight.at[n, pl.ds(start, width)], weight_sem.at[n, k],
            )
            for k, (start, width) in enumerate(spans)
        ]
        for n, kind in enumerate(kinds)
    ]
    with jax.named_scope("hid"):
        g = gate[...].astype(jnp.float32)
        u = upper[...].astype(jnp.float32)
        sig = jax.nn.sigmoid(g)
        hidden_ref[chip, core] = (g * sig * u).astype(jnp.bfloat16)
        act_ref[...] = g * sig
        slope_ref[...] = u * sig * (1.0 + g * (1.0 - sig))
    for k, (start, width) in enumerate(pieces):
        piece = hidden_ref.at[chip, core, :, pl.ds(start, width)]
        for other in chips:
            send(piece, hidden_sem.at[k, chip, core], (other * CORES + core, t))
    send(hidden_ref.at[chip, core], pair_sem.at[0], (mate, t))
    for loads_of in weight_loads:
        for load in loads_of:
            load.start()
    cols_ref[chip, core, t] = mine[:, block_of(dp)]
    for other in chips:
        extra[other, core, t] = mine[:, block_of(other * CORES + core)]

    def own_line(i):
        source = at(line[i], b)
        block = cols_ref.at[chip, :, source]
        arrived(block, own_sem.at[source])
        if i == 0:
            for c in range(CORES):
                relay(cols_ref.at[chip, c, source], own_sem.at[source], own_slots[c])
        for side in sides:
            send(block, own_sem.at[source], (dp, at(a, side)))

    def extra_line(i):
        source = at(line[i], b)
        for n, other in enumerate(chips):
            for c in range(CORES):
                block = extra.at[other, c, source]
                arrived(block, extra_sem.at[other, c, source])
                if i == 0:
                    relay(block, extra_sem.at[other, c, source], extra_slots[n][c])
                if c == 0:
                    for side in sides:
                        send(block, extra_sem.at[other, c, source], (dp, at(a, side)))
            if i == 2:
                block = extra.at[other, :, source]
                send(block, far_sem.at[chip, b], (other * CORES + core, t), cols_ref.at[chip, :, source])

    def extra_side():
        slots = []
        for side in sides:
            for other in chips:
                source = at(a, side)
                block = extra.at[other, 1, source]
                arrived(block, extra_sem.at[other, 1, source])
                slots.append(spread(block, extra_sem.at[other, 1, source], dp))
        return slots

    def extra_relay():
        n = 0
        for side in sides:
            for other in chips:
                source = at(mirror, side)
                block, sem = extra.at[other, 1, source], extra_sem.at[other, 1, source]

                @pl.when(between == 1)
                def _():
                    arrived(block, sem)

                relay(block, sem, side_slots[n])
                n += 1

    def own_last():
        for side in sides:
            for step in [a] + line:
                source = at(step, side)
                arrived(cols_ref.at[chip, :, source], own_sem.at[source])
        arrived(cols_ref.at[chip, 1 - core, t], own_sem.at[t])

    def extra_last():
        for side in sides:
            for other in chips:
                arrived(extra.at[other, 0, at(a, side)], extra_sem.at[other, 0, at(a, side)])
                for i, step in enumerate(line):
                    source = at(step, side)
                    arrived(extra.at[other, 0, source], extra_sem.at[other, 0, source])
                    block, sem = extra.at[other, 1, source], extra_sem.at[other, 1, source]
                    if i == 0:

                        @pl.when(between == 0)
                        def _():
                            arrived(block, sem)
                    else:
                        arrived(block, sem)
                    if i == 2:
                        block = extra.at[other, :, source]
                        send(block, far_sem.at[chip, side], (other * CORES + core, t), cols_ref.at[chip, :, source])
        for other in chips:
            arrived(extra.at[other, 1 - core, t], extra_sem.at[other, 1 - core, t])

    def cols_own():
        for other in chips:
            for c in range(CORES):
                arrived(cols_ref.at[other, c, t], cross_sem.at[other, c])
            block = cols_ref.at[other, :, t]
            for side in sides:
                send(block, cols_sem.at[0, other, t], (dp, at(a, side)))
            if has_line:
                for step in (twin, mirror):
                    send(block, cols_sem.at[0, other, t], (dp, at(step, b)))

    def cols_line(i):
        source = at(line[i], b)
        for other in chips:
            sem = cols_sem.at[0, other, source]
            arrived(cols_ref.at[other, :, source], sem)
            for side in sides:
                send(cols_ref.at[other, 0, source], sem, (dp, at(a, side)))

    def cols_side():
        for side in sides:
            for other in chips:
                source = at(a, side)
                arrived(cols_ref.at[other, :, source], cols_sem.at[0, other, source])
                if has_line:
                    send_two(
                        cols_ref.at[other, 1, source], cols_sem.at[1, other, source], [(dp, at(twin, b)), (dp, at(mirror, b))]
                    )

    def cols_last():
        for other in chips:
            for side in sides:
                for step in line[:2]:
                    source = at(step, side)
                    arrived(cols_ref.at[other, 0, source], cols_sem.at[0, other, source])
                    arrived(cols_ref.at[other, 1, source], cols_sem.at[1, other, source])
            if has_line:
                for side in [b] + sides:
                    source = at(across, side)
                    arrived(cols_ref.at[other, :, source], far_sem.at[other, side])

    def hidden_piece(k):
        start, width = pieces[k]
        for other in chips:
            piece = hidden_ref.at[other, core, :, pl.ds(start, width)]
            arrived(piece, hidden_sem.at[k, other, core])
            send(piece, hidden_sem.at[k, other, core], (mate, t))

    def scoped(name, job, *args):
        with jax.named_scope(name):
            return job(*args)

    if has_line:
        scoped("own_line0", own_line, 0)
        scoped("own_line1", own_line, 1)
    side_slots = scoped("extra_side", extra_side)
    if has_line:
        scoped("own_line2", own_line, 2)
    scoped("cols_own", cols_own)
    for i in range(len(line)):
        scoped("extra_line%d" % i, extra_line, i)
    scoped("own_last", own_last)

    jobs = [("extra_relay", extra_relay)] if has_line else []
    jobs += [("cols_side", cols_side)]
    jobs += [("cols_line%d" % i, functools.partial(cols_line, i)) for i in range(len(line[:2]))]
    late = [("hidden%d" % k, functools.partial(hidden_piece, k)) for k in range(len(pieces))]
    group = n_t * depth
    for n, kind in enumerate(kinds):
        if n == 1:
            for job in jobs:
                scoped(*job)
            scoped("extra_last", extra_last)
            jobs = late
        blocks = cols_ref if n == 0 else extra
        for k, owner in enumerate((core, 1 - core)):
            left[pl.ds(k * group, group)] = (
                blocks[kind, owner].astype(jnp.float32).reshape(group, feats).astype(jnp.bfloat16)
            )
        for k, (start, width) in enumerate(spans):
            span = pl.ds(start, width)
            with jax.named_scope("w#n=%d" % n):
                weight_loads[n][k].wait()
            with jax.named_scope("dot#n=%d" % n):
                term = lax.dot_general(
                    left[...], weight[n, span], (((1,), (1,)), ((), ())), preferred_element_type=jnp.float32
                )
                if n > 0:
                    term = acc[:, span] + term
                if n < len(kinds) - 1:
                    acc[:, span] = term
                else:
                    grad_ref[:, span] = term[:group]
                    leave[:, span] = term[group:].astype(jnp.bfloat16)
            if n == len(kinds) - 1:
                send(leave.at[:, span], grad_sem.at[k], (mate, t), other_ref.at[:, span])
            if jobs:
                scoped(*jobs.pop(0))
    for job in jobs:
        scoped(*job)

    with jax.named_scope("tail_cols"):
        cols_last()
    with jax.named_scope("tail_hid"):
        for k, (start, width) in enumerate(pieces):
            for other in chips:
                arrived(hidden_ref.at[other, 1 - core, :, pl.ds(start, width)], hidden_sem.at[k, other, 1 - core])
        arrived(hidden_ref.at[chip, 1 - core], pair_sem.at[0])
    with jax.named_scope("tail_grad"):
        for k, (start, width) in enumerate(spans):
            arrived(other_ref.at[:, pl.ds(start, width)], grad_sem.at[k])
    with jax.named_scope("tail_send"):
        for copy in sent:
            copy.wait_send()


def finish_kernel(
    spans, cols_ref, hidden_ref, grad_ref, other_ref, act_ref, slope_ref,
    weight_out, gate_out, up_out, turned, gate, upper, weight_sem, grad_sem,
):
    copies = []
    for k, (start, width) in enumerate(spans):
        span = pl.ds(start, width)
        turned[span] = lax.dot_general(
            hidden_ref[:, span], cols_ref[...], (((0,), (0,)), ((), ())), preferred_element_type=jnp.float32
        )
        copies.append(pltpu.make_async_copy(turned.at[span], weight_out.at[span], weight_sem.at[k]))
        copies[-1].start()
        if k == 0:
            grad = grad_ref[...] + other_ref[...].astype(jnp.float32)
            upper[...] = (grad * act_ref[...]).astype(jnp.bfloat16)
            gate[...] = (grad * slope_ref[...]).astype(jnp.bfloat16)
            copies.append(pltpu.make_async_copy(upper, up_out, grad_sem.at[0]))
            copies.append(pltpu.make_async_copy(gate, gate_out, grad_sem.at[1]))
            copies[-2].start()
            copies[-1].start()
    for copy in copies:
        copy.wait()


def body(n_dp, n_t, grad_out, gate_pre, up_pre, down_weight):
    depth, model = grad_out.shape
    group, wide = gate_pre.shape
    feats = model // n_dp
    n_chip = n_dp // CORES
    outer = 4 if n_t % 4 == 0 else 1
    inner = n_t // outer
    spans = cut(wide, 512)
    pieces = cut(wide, 1024)
    n_line, n_side, n_other = outer - 1, inner - 1, n_chip - 1
    n_send = (
        n_other * CORES + n_chip * (CORES * (n_side + 2) + 1) + 2 * len(pieces) * n_other + 1
        + n_line * n_side + n_other * (n_line * n_side + 1 + 3 * n_side)
        + n_other * (n_side + 2 + 3 * n_side) + len(spans)
    )
    lanes = pl.cdiv(wide, 128) * 128
    results = 2 * n_dp * group * (feats + lanes) + (3 * 4 + 2) * group * lanes
    limit = VMEM - results - 64 * 1024
    anywhere = pl.BlockSpec(memory_space=pltpu.HBM)
    vmem = pl.BlockSpec(memory_space=pltpu.VMEM)
    dma = pltpu.SemaphoreType.DMA
    cols, hidden, *factors = pl.pallas_call(
        functools.partial(gather_kernel, n_dp, n_t, outer, spans, pieces),
        out_shape=[
            pltpu.VMEM((n_chip, CORES, n_t, depth, feats), jnp.bfloat16),
            pltpu.VMEM((n_chip, CORES, group, wide), jnp.bfloat16),
            pltpu.VMEM((group, wide), jnp.float32),
            pltpu.VMEM((group, wide), jnp.bfloat16),
            pltpu.VMEM((group, wide), jnp.float32),
            pltpu.VMEM((group, wide), jnp.float32),
        ],
        in_specs=[anywhere] * 4,
        out_specs=[vmem] * 6,
        scratch_shapes=[
            pltpu.VMEM((depth, model), jnp.bfloat16),
            pltpu.VMEM((n_chip, CORES, n_t, depth, feats), jnp.bfloat16),
            pltpu.VMEM((group, wide), jnp.bfloat16),
            pltpu.VMEM((group, wide), jnp.bfloat16),
            pltpu.VMEM((n_chip, wide, feats), jnp.bfloat16),
            pltpu.VMEM((CORES * group, feats), jnp.bfloat16),
            pltpu.VMEM((CORES * group, wide), jnp.float32),
            pltpu.VMEM((group, wide), jnp.bfloat16),
            dma((3,)),
            dma((n_chip, len(spans))),
            dma((n_send,)),
            dma((n_t,)),
            dma((n_chip, CORES, n_t)),
            dma((n_chip, CORES)),
            dma((2, n_chip, n_t)),
            dma((n_chip, inner)),
            dma((len(pieces), n_chip, CORES)),
            dma((1,)),
            dma((len(spans),)),
        ],
        compiler_params=pltpu.CompilerParams(collective_id=0, has_side_effects=True, vmem_limit_bytes=limit),
    )(grad_out, gate_pre, up_pre, down_weight.T)
    cols = cols.reshape(n_dp * group, feats)
    hidden = hidden.reshape(n_dp * group, wide)

    steps = [(0, min(128, wide))] + [(128 + start, width) for start, width in cut(wide - 128, 256)]
    turned, grad_gate, grad_up = pl.pallas_call(
        functools.partial(finish_kernel, steps),
        out_shape=[
            jax.ShapeDtypeStruct((wide, feats), jnp.float32),
            jax.ShapeDtypeStruct((group, wide), jnp.bfloat16),
            jax.ShapeDtypeStruct((group, wide), jnp.bfloat16),
        ],
        in_specs=[vmem] * 6,
        out_specs=[anywhere] * 3,
        scratch_shapes=[
            pltpu.VMEM((wide, feats), jnp.float32),
            pltpu.VMEM((group, wide), jnp.bfloat16),
            pltpu.VMEM((group, wide), jnp.bfloat16),
            dma((len(steps),)),
            dma((2,)),
        ],
        compiler_params=pltpu.CompilerParams(vmem_limit_bytes=limit),
    )(*[pltpu.with_memory_space_constraint(x, pltpu.VMEM) for x in (cols, hidden, *factors)])
    return turned.T, grad_gate, grad_up


def solution(mesh):
    in_specs = (P(("dp", "tensor"), None), P("dp", "tensor"), P("dp", "tensor"), P(None, "tensor"))
    out_specs = (P("dp", "tensor"), P("dp", "tensor"), P("dp", "tensor"))
    fn = functools.partial(body, mesh.shape["dp"], mesh.shape["tensor"])
    return jax.shard_map(fn, mesh=mesh, in_specs=in_specs, out_specs=out_specs, check_vma=False)
```

```python
import functools

import jax
import jax.numpy as jnp
from jax import lax
from jax.experimental import pallas as pl
from jax.experimental.pallas import tpu as pltpu
from jax.sharding import PartitionSpec as P

MESH = pl.DeviceIdType.MESH
CORES = 2
VMEM = 67043328
MIDDLE, END = "middle", "end"
ORDER = (
    ("own", 0),
    ("own", 1, MIDDLE),
    ("cols",),
    ("extra", 0),
    ("extra", 1, MIDDLE),
    ("sides",),
    ("own", 2),
    ("own", 1, END),
    ("extra", 2),
    ("extra", 1, END),
    ("hidden", 0),
    ("owns",),
    ("dots", 0),
    ("hidden", 1),
    ("dots", 1),
    ("extras",),
)


def cut(wide, step):
    return [(start, min(step, wide - start)) for start in range(0, wide, step)]


def gather_kernel(
    n_dp, n_t, outer, spans, pieces,
    go_hbm, gate_hbm, up_hbm, weight_hbm,
    cols_ref, hidden_ref, grad_ref, other_ref, act_ref, slope_ref, extra, distant,
    mine, gate, upper, weight, left, leave, gauge,
    load_sem, weight_sem, send_sem, ready_sem, own_sem, extra_sem, cols_sem, hidden_sem,
):
    inner = n_t // outer
    n_chip = n_dp // CORES
    depth, feats = mine.shape[0], cols_ref.shape[-1]
    group = n_t * depth
    dp, t = lax.axis_index("dp"), lax.axis_index("tensor")
    chip, core = dp // CORES, dp % CORES
    mate = chip * CORES + (1 - core)
    a, b = t // inner, t % inner
    chips = [lax.rem(chip + d, n_chip) for d in range(1, n_chip)]
    sides = [lax.rem(b + d, inner) for d in range(1, inner)]
    n_other, n_side = len(chips), len(sides)

    has_line = outer == 4
    middle = (a * (3 - a)) // 2
    twin, mirror, across = a + 1 - 2 * (a % 2), 3 - a, (a + 2) % 4
    second = middle * mirror + (1 - middle) * across
    third = middle * across + (1 - middle) * mirror
    line = [twin, second, third] if has_line else []
    n_line = len(line)

    own_joint = own_sem.at[outer]
    cross, from_sides, late = (cols_sem.at[k] for k in range(3))

    def own_line_sem(step):
        return own_sem.at[step]

    def extra_line_sem(other, step):
        return extra_sem.at[other, step]

    def extra_joint(other):
        return extra_sem.at[other, outer]

    def at(step, side):
        return step * inner + side

    loads = [
        pltpu.make_async_copy(go_hbm, mine, load_sem.at[0]),
        pltpu.make_async_copy(gate_hbm, gate, load_sem.at[1]),
        pltpu.make_async_copy(up_hbm, upper, load_sem.at[2]),
    ]
    for load in loads:
        load.start()

    barrier = pltpu.get_barrier_semaphore()
    peers = [(lax.rem(dp + d, n_dp), t) for d in range(1, n_dp)]
    for c in range(CORES):
        peers += [(chip * CORES + c, at(a, side)) for side in sides]
        if has_line:
            peers.append((chip * CORES + c, at(twin, b)))
    for peer in peers:
        pl.semaphore_signal(barrier, inc=1, device_id=peer, device_id_type=MESH)
    if has_line:

        @pl.when(middle == 1)
        def _():
            for c in range(CORES):
                pl.semaphore_signal(barrier, inc=1, device_id=(chip * CORES + c, at(mirror, b)), device_id_type=MESH)

    with jax.named_scope("go"):
        loads[0].wait()
    with jax.named_scope("barrier"):
        pl.semaphore_wait(barrier, len(peers) + (CORES * middle if has_line else 0))

    if has_line:

        @pl.when(middle == 1)
        def _():
            pl.semaphore_signal(ready_sem.at[0], inc=1, device_id=(dp, at(mirror, b)), device_id_type=MESH)

    sent, sent_middle, sent_end = [], [], []

    def copy_to(block, sem, peer, dst=None, lane=0):
        return pltpu.make_async_remote_copy(
            src_ref=block, dst_ref=block if dst is None else dst, send_sem=send_sem.at[lane], recv_sem=sem,
            device_id=peer, device_id_type=MESH,
        )

    def arrived(blocks, sem):
        copy_to(gauge.at[pl.ds(0, blocks)], sem, (mate, t)).wait_recv()

    def block_of(group):
        return pl.ds(pl.multiple_of(group * feats, feats), feats)

    def blocks_in(block):
        size = 1
        for dim in block.shape:
            size *= dim
        return size // (depth * feats)

    def send(block, sem, peer, dst=None):
        sent.append(blocks_in(block))
        copy_to(block, sem, peer, dst).start()

    def send_middle(block, sem, peer, dst=None):
        sent_middle.append(blocks_in(block))

        @pl.when(middle == 1)
        def _():
            copy_to(block, sem, peer, dst).start()

    for other in chips:
        for c in range(CORES):
            group_of = other * CORES + c
            send(mine.at[:, block_of(group_of)], cross, (group_of, t), cols_ref.at[chip, core, t])

    def send_end(block, sem, peer, dst=None):
        sent_end.append(blocks_in(block))

        @pl.when(middle == 0)
        def _():
            copy_to(block, sem, peer, dst).start()

    def pair_of(other):
        return pl.ds(pl.multiple_of(other * CORES * feats, CORES * feats), CORES * feats)

    def own_block(source, dst, line_sem, joint):
        for c in range(CORES):
            target = chip * CORES + c
            block = mine.at[:, block_of(source * CORES + c)]
            for side in sides:
                send(block, joint, (target, at(a, side)), dst)
            if has_line:
                send(block, line_sem, (target, at(twin, b)), dst)
                send_middle(block, line_sem, (target, at(mirror, b)), dst)
        send(mine.at[:, block_of(source * CORES + 1 - core)], joint, (mate, t), dst)

    own_block(chip, cols_ref.at[chip, core, t], own_line_sem(a), own_joint)
    for n, other in enumerate(chips):
        block = mine.at[:, pair_of(other)]
        for side in sides:
            send(block, extra_joint(n), (dp, at(a, side)), extra.at[n, t])
        if has_line:
            send(block, extra_line_sem(n, a), (dp, at(twin, b)), extra.at[n, t])
            send_middle(block, extra_line_sem(n, a), (dp, at(mirror, b)), extra.at[n, t])

    def own_far():
        @pl.when(middle == 1)
        def _():
            pl.semaphore_wait(ready_sem.at[0], 1)
            pl.semaphore_signal(ready_sem.at[1], inc=1, device_id=(dp, at(twin, b)), device_id_type=MESH)

        @pl.when(middle == 0)
        def _():
            pl.semaphore_wait(ready_sem.at[1], 1)

        for c in range(CORES):
            block = mine.at[:, block_of(chip * CORES + c)]
            send_end(block, own_line_sem(a), (chip * CORES + c, at(mirror, b)), cols_ref.at[chip, core, t])
        for n, other in enumerate(chips):
            send_end(mine.at[:, pair_of(other)], extra_line_sem(n, a), (dp, at(mirror, b)), extra.at[n, t])

    with jax.named_scope("hid_load"):
        loads[1].wait()
        loads[2].wait()
    weight_loads = [
        pltpu.make_async_copy(
            weight_hbm.at[pl.ds(start, width), block_of(dp)], weight.at[pl.ds(start, width)], weight_sem.at[k],
        )
        for k, (start, width) in enumerate(spans)
    ]
    weight_loads += [
        pltpu.make_async_copy(weight_hbm.at[:, pair_of(other)], distant.at[n], weight_sem.at[len(spans) + n])
        for n, other in enumerate(chips)
    ]
    with jax.named_scope("hid"):
        g = gate[...].astype(jnp.float32)
        u = upper[...].astype(jnp.float32)
        sig = jax.nn.sigmoid(g)
        hidden_ref[chip, core] = (g * sig * u).astype(jnp.bfloat16)
        act_ref[...] = g * sig
        slope_ref[...] = u * sig * (1.0 + g * (1.0 - sig))
    hidden_mate, grad_mate = hidden_sem.at[len(pieces)], hidden_sem.at[len(pieces) + 1]
    for k, (start, width) in enumerate(pieces):
        piece = hidden_ref.at[chip, core, :, pl.ds(start, width)]
        for other in chips:
            copy_to(piece, hidden_sem.at[k], (other * CORES + core, t), lane=1).start()
    copy_to(hidden_ref.at[chip, core], hidden_mate, (mate, t), lane=1).start()
    for load in weight_loads:
        load.start()
    if has_line:
        with jax.named_scope("own_far"):
            own_far()
    cols_ref[chip, core, t] = mine[:, block_of(dp)]
    for n, other in enumerate(chips):
        extra[n, t] = mine[:, pair_of(other)]

    def onward(i):
        return (dp, at(mirror if i == 0 else twin, b))

    def only(job):
        counted = set()

        def run(*args, where=None):
            kept = list(sent), list(sent_middle), list(sent_end)
            if where is None:
                job(*args)
            else:
                pl.when(middle == where)(functools.partial(job, *args))
            if args in counted:
                sent[:], sent_middle[:], sent_end[:] = kept
            counted.add(args)

        return run

    @only
    def own_line(i):
        block, sem = cols_ref.at[chip, :, at(line[i], b)], own_line_sem(line[i])
        arrived(CORES, sem)
        if i < 2:
            send_middle(block, sem, onward(i))
        for side in sides:
            send(block, own_joint, (dp, at(a, side)))

    @only
    def extra_line(i):
        source = at(line[i], b)
        for n, other in enumerate(chips):
            block, sem = extra.at[n, source], extra_line_sem(n, line[i])
            arrived(CORES, sem)
            if i < 2:
                send_middle(block, sem, onward(i))
            for side in sides:
                send(block, extra_joint(n), (dp, at(a, side)))
            if i == 2:
                for c in range(CORES):
                    block = extra.at[n, source, :, pl.ds(c * feats, feats)]
                    for side in [b] + sides:
                        send(block, late, (other * CORES + c, at(a, side)), cols_ref.at[chip, core, source])

    @only
    def own_last():
        arrived(n_side * (1 + n_line) * CORES + 1, own_joint)

    @only
    def extra_last():
        for n in range(n_other):
            arrived(n_side * (1 + n_line) * CORES, extra_joint(n))

    def cols_along(side):
        for other in chips:
            block = cols_ref.at[other, :, at(a, side)]
            send(block, late, (dp, at(twin, b)))
            send_middle(block, late, (dp, at(mirror, b)))
            send_middle(block, late, (dp, at(across, b)))

    @only
    def cols_own():
        arrived(n_other * CORES, cross)
        for other in chips:
            for side in sides:
                send(cols_ref.at[other, :, t], from_sides, (dp, at(a, side)))
        if has_line:
            cols_along(b)

    @only
    def cols_sides():
        if n_side:
            arrived(n_other * n_side * CORES, from_sides)
        if has_line:
            for side in sides:
                cols_along(side)

    def cols_last():
        if has_line:
            arrived(3 * n_other * (1 + n_side) * CORES, late)

    @only
    def hidden_piece(k):
        start, width = pieces[k]
        for other in chips:
            piece = hidden_ref.at[other, core, :, pl.ds(start, width)]
            copy_to(piece, hidden_sem.at[k], (mate, t), lane=1).wait_recv()
        for other in chips:
            piece = hidden_ref.at[other, core, :, pl.ds(start, width)]
            copy_to(piece, hidden_mate, (mate, t), lane=1).start()

    def scoped(name, job, *args):
        with jax.named_scope(name):
            return job(*args)

    def dot(k):
        if k >= len(spans):
            return
        if k == 0:
            for place, owner in enumerate((core, 1 - core)):
                left[pl.ds(place * group, group)] = (
                    cols_ref[chip, owner].astype(jnp.float32).reshape(group, feats).astype(jnp.bfloat16)
                )
        start, width = spans[k]
        span = pl.ds(start, width)
        weight_loads[k].wait()
        term = lax.dot_general(
            left[...], weight[span], (((1,), (1,)), ((), ())), preferred_element_type=jnp.float32
        )
        grad_ref[:, span] = term[:group]
        leave[:, span] = term[group:].astype(jnp.bfloat16)
        copy_to(leave.at[:, span], grad_mate, (mate, t), other_ref.at[:, span], 1).start()

    jobs = {
        "own": own_line, "extra": extra_line, "cols": cols_own, "sides": cols_sides,
        "owns": own_last, "extras": extra_last, "hidden": hidden_piece, "dots": dot,
    }
    line_jobs = ("own", "extra")
    for name, *rest in ORDER:
        if name in line_jobs and not has_line or name == "hidden" and rest[0] >= len(pieces):
            continue
        where = rest.pop() if rest and rest[-1] in (MIDDLE, END) else None
        if where is None:
            scoped(name + "".join(map(str, rest)), jobs[name], *rest)
        else:
            scoped(name + "".join(map(str, rest)) + where[0], functools.partial(jobs[name], where=int(where == MIDDLE)), *rest)

    for load in weight_loads[len(spans):]:
        load.wait()
    with jax.named_scope("tail_cols"):
        cols_last()
    with jax.named_scope("tail_hid"):
        everyone = hidden_ref.at[:, 1 - core]
        copy_to(everyone, hidden_mate, (mate, t), lane=1).wait_recv()
    with jax.named_scope("tail_grad"):
        copy_to(leave, grad_mate, (mate, t), other_ref, 1).wait_recv()
    with jax.named_scope("tail_send"):
        copy_to(gauge.at[pl.ds(0, sum(sent))], late, (mate, t)).wait_send()
        if has_line:

            @pl.when(middle == 1)
            def _():
                copy_to(gauge.at[pl.ds(0, sum(sent_middle))], late, (mate, t)).wait_send()

            @pl.when(middle == 0)
            def _():
                copy_to(gauge.at[pl.ds(0, sum(sent_end))], late, (mate, t)).wait_send()

        copy_to(hidden_ref, hidden_mate, (mate, t), lane=1).wait_send()


def finish_kernel(
    spans, chunks, cols_ref, hidden_ref, grad_ref, other_ref, act_ref, slope_ref, extra_ref, distant_ref,
    weight_out, gate_out, up_out, turned, gate, upper, left, weight_sem, grad_sem,
):
    copies = []

    def leave(src, dst, sem):
        copies.append(pltpu.make_async_copy(src, dst, sem))
        copies[-1].start()

    for k, (start, width) in enumerate(spans):
        span = pl.ds(start, width)
        turned[span] = lax.dot_general(
            hidden_ref[:, span], cols_ref[...], (((0,), (0,)), ((), ())), preferred_element_type=jnp.float32
        )
        leave(turned.at[span], weight_out.at[span], weight_sem.at[k])
    n_other, _, _, pair = extra_ref.shape
    for n in range(n_other):
        left[n] = extra_ref[n].astype(jnp.float32).reshape(left.shape[1], pair).astype(jnp.bfloat16)
    for k, (start, width) in enumerate(chunks):
        span = pl.ds(start, width)
        grad = grad_ref[:, span] + other_ref[:, span].astype(jnp.float32)
        for n in range(n_other):
            grad += lax.dot_general(
                left[n], distant_ref[n, span], (((1,), (1,)), ((), ())), preferred_element_type=jnp.float32
            )
        upper[:, span] = (grad * act_ref[:, span]).astype(jnp.bfloat16)
        gate[:, span] = (grad * slope_ref[:, span]).astype(jnp.bfloat16)
    leave(upper, up_out, grad_sem.at[0])
    leave(gate, gate_out, grad_sem.at[1])
    for copy in copies:
        copy.wait()


def body(n_dp, n_t, grad_out, gate_pre, up_pre, down_weight):
    depth, model = grad_out.shape
    group, wide = gate_pre.shape
    feats = model // n_dp
    n_chip = n_dp // CORES
    outer = 4 if n_t % 4 == 0 else 1
    inner = n_t // outer
    spans = cut(wide, 1024)
    pieces = cut(wide, 1024)
    n_side, n_other = inner - 1, n_chip - 1
    n_gauge = (n_chip + 1) * (n_side + 4) * 2 + 3 * n_side * 2 + n_other * (16 * n_side + 12)
    lanes = pl.cdiv(wide, 128) * 128
    pair = CORES * feats
    results = 2 * (n_dp * group * (feats + lanes) + 7 * group * lanes + n_other * (group + wide) * pair)
    limit = VMEM - results - 64 * 1024
    anywhere = pl.BlockSpec(memory_space=pltpu.HBM)
    vmem = pl.BlockSpec(memory_space=pltpu.VMEM)
    dma = pltpu.SemaphoreType.DMA
    cols, hidden, *factors = pl.pallas_call(
        functools.partial(gather_kernel, n_dp, n_t, outer, spans, pieces),
        out_shape=[
            pltpu.VMEM((n_chip, CORES, n_t, depth, feats), jnp.bfloat16),
            pltpu.VMEM((n_chip, CORES, group, wide), jnp.bfloat16),
            pltpu.VMEM((group, wide), jnp.float32),
            pltpu.VMEM((group, wide), jnp.bfloat16),
            pltpu.VMEM((group, wide), jnp.float32),
            pltpu.VMEM((group, wide), jnp.float32),
            pltpu.VMEM((n_other, n_t, depth, pair), jnp.bfloat16),
            pltpu.VMEM((n_other, wide, pair), jnp.bfloat16),
        ],
        in_specs=[anywhere] * 4,
        out_specs=[vmem] * 8,
        scratch_shapes=[
            pltpu.VMEM((depth, model), jnp.bfloat16),
            pltpu.VMEM((group, wide), jnp.bfloat16),
            pltpu.VMEM((group, wide), jnp.bfloat16),
            pltpu.VMEM((wide, feats), jnp.bfloat16),
            pltpu.VMEM((CORES * group, feats), jnp.bfloat16),
            pltpu.VMEM((group, wide), jnp.bfloat16),
            pltpu.VMEM((n_gauge, depth, feats), jnp.bfloat16),
            dma((3,)),
            dma((len(spans) + n_other,)),
            dma((2,)),
            pltpu.SemaphoreType.REGULAR((2,)),
            dma((outer + 1,)),
            dma((n_other, outer + 1)),
            dma((3,)),
            dma((len(pieces) + 2,)),
        ],
        compiler_params=pltpu.CompilerParams(collective_id=0, has_side_effects=True, vmem_limit_bytes=limit),
    )(grad_out, gate_pre, up_pre, down_weight.T)
    cols = cols.reshape(n_dp * group, feats)
    hidden = hidden.reshape(n_dp * group, wide)

    steps = [(0, min(128, wide))] + [(128 + start, width) for start, width in cut(wide - 128, 256)]
    turned, grad_gate, grad_up = pl.pallas_call(
        functools.partial(finish_kernel, steps, cut(wide, 512)),
        out_shape=[
            jax.ShapeDtypeStruct((wide, feats), jnp.float32),
            jax.ShapeDtypeStruct((group, wide), jnp.bfloat16),
            jax.ShapeDtypeStruct((group, wide), jnp.bfloat16),
        ],
        in_specs=[vmem] * 8,
        out_specs=[anywhere] * 3,
        scratch_shapes=[
            pltpu.VMEM((wide, feats), jnp.float32),
            pltpu.VMEM((group, wide), jnp.bfloat16),
            pltpu.VMEM((group, wide), jnp.bfloat16),
            pltpu.VMEM((n_other, group, pair), jnp.bfloat16),
            dma((len(steps),)),
            dma((2,)),
        ],
        compiler_params=pltpu.CompilerParams(vmem_limit_bytes=limit),
    )(*[pltpu.with_memory_space_constraint(x, pltpu.VMEM) for x in (cols, hidden, *factors)])
    return turned.T, grad_gate, grad_up


def solution(mesh):
    in_specs = (P(("dp", "tensor"), None), P("dp", "tensor"), P("dp", "tensor"), P(None, "tensor"))
    out_specs = (P("dp", "tensor"), P("dp", "tensor"), P("dp", "tensor"))
    fn = functools.partial(body, mesh.shape["dp"], mesh.shape["tensor"])
    return jax.shard_map(fn, mesh=mesh, in_specs=in_specs, out_specs=out_specs, check_vma=False)
```

```python
import functools

import jax
import jax.numpy as jnp
from jax import lax
from jax.experimental import pallas as pl
from jax.experimental.pallas import tpu as pltpu
from jax.sharding import PartitionSpec as P

MESH = pl.DeviceIdType.MESH
CORES = 2
VMEM = 67043328
SLICE = 512
TURNS = 4
MIDDLE, END = "middle", "end"
ORDER = (
    ("own", 0),
    ("own", 1, MIDDLE),
    ("cols",),
    ("extra", 0),
    ("extra", 1, MIDDLE),
    ("turn", 0),
    ("turn", 1),
    ("turn", 2),
    ("turn", 3),
    ("sides",),
    ("own", 2),
    ("own", 1, END),
    ("extra", 2),
    ("turn", 4),
    ("extra", 1, END),
    ("hidden", 0),
    ("owns",),
    ("dots", 0),
    ("hidden", 1),
    ("dots", 1),
    ("extras",),
)


def cut(wide, step):
    return [(start, min(step, wide - start)) for start in range(0, wide, step)]


def gather_kernel(
    n_dp, n_t, outer, spans, pieces,
    go_hbm, gate_hbm, up_hbm, weight_hbm,
    cols_ref, hidden_ref, grad_ref, other_ref, act_ref, slope_ref, extra, distant,
    mine, gate, upper, weight, flat, plain, left, leave, gauge,
    load_sem, weight_sem, send_sem, ready_sem, own_sem, extra_sem, cols_sem, hidden_sem,
):
    inner = n_t // outer
    n_chip = n_dp // CORES
    depth, feats = mine.shape[0], cols_ref.shape[-1]
    group = n_t * depth
    dp, t = lax.axis_index("dp"), lax.axis_index("tensor")
    chip, core = dp // CORES, dp % CORES
    mate = chip * CORES + (1 - core)
    a, b = t // inner, t % inner
    chips = [lax.rem(chip + d, n_chip) for d in range(1, n_chip)]
    sides = [lax.rem(b + d, inner) for d in range(1, inner)]
    n_other, n_side = len(chips), len(sides)

    has_line = outer == 4
    middle = (a * (3 - a)) // 2
    twin, mirror, across = a + 1 - 2 * (a % 2), 3 - a, (a + 2) % 4
    second = middle * mirror + (1 - middle) * across
    third = middle * across + (1 - middle) * mirror
    line = [twin, second, third] if has_line else []
    n_line = len(line)

    own_joint = own_sem.at[outer]
    cross, from_sides, late = (cols_sem.at[k] for k in range(3))

    def own_line_sem(step):
        return own_sem.at[step]

    def extra_line_sem(other, step):
        return extra_sem.at[other, step]

    def extra_joint(other):
        return extra_sem.at[other, outer]

    def at(step, side):
        return step * inner + side

    loads = [
        pltpu.make_async_copy(go_hbm, mine, load_sem.at[0]),
        pltpu.make_async_copy(gate_hbm, gate, load_sem.at[1]),
        pltpu.make_async_copy(up_hbm, upper, load_sem.at[2]),
    ]
    for load in loads:
        load.start()

    barrier = pltpu.get_barrier_semaphore()
    peers = [(lax.rem(dp + d, n_dp), t) for d in range(1, n_dp)]
    for c in range(CORES):
        peers += [(chip * CORES + c, at(a, side)) for side in sides]
        if has_line:
            peers.append((chip * CORES + c, at(twin, b)))
    for peer in peers:
        pl.semaphore_signal(barrier, inc=1, device_id=peer, device_id_type=MESH)
    if has_line:

        @pl.when(middle == 1)
        def _():
            for c in range(CORES):
                pl.semaphore_signal(barrier, inc=1, device_id=(chip * CORES + c, at(mirror, b)), device_id_type=MESH)

    with jax.named_scope("go"):
        loads[0].wait()
    with jax.named_scope("barrier"):
        pl.semaphore_wait(barrier, len(peers) + (CORES * middle if has_line else 0))

    if has_line:

        @pl.when(middle == 1)
        def _():
            pl.semaphore_signal(ready_sem.at[0], inc=1, device_id=(dp, at(mirror, b)), device_id_type=MESH)

    sent, sent_middle, sent_end = [], [], []

    def copy_to(block, sem, peer, dst=None, lane=0):
        return pltpu.make_async_remote_copy(
            src_ref=block, dst_ref=block if dst is None else dst, send_sem=send_sem.at[lane], recv_sem=sem,
            device_id=peer, device_id_type=MESH,
        )

    def arrived(blocks, sem):
        copy_to(gauge.at[pl.ds(0, blocks)], sem, (mate, t)).wait_recv()

    def block_of(group):
        return pl.ds(pl.multiple_of(group * feats, feats), feats)

    def blocks_in(block):
        size = 1
        for dim in block.shape:
            size *= dim
        return size // (depth * feats)

    def send(block, sem, peer, dst=None):
        sent.append(blocks_in(block))
        copy_to(block, sem, peer, dst).start()

    def send_middle(block, sem, peer, dst=None):
        sent_middle.append(blocks_in(block))

        @pl.when(middle == 1)
        def _():
            copy_to(block, sem, peer, dst).start()

    for other in chips:
        for c in range(CORES):
            group_of = other * CORES + c
            send(mine.at[:, block_of(group_of)], cross, (group_of, t), cols_ref.at[chip, core, t])

    def send_end(block, sem, peer, dst=None):
        sent_end.append(blocks_in(block))

        @pl.when(middle == 0)
        def _():
            copy_to(block, sem, peer, dst).start()

    def pair_of(other):
        return pl.ds(pl.multiple_of(other * CORES * feats, CORES * feats), CORES * feats)

    def own_block(source, dst, line_sem, joint):
        for c in range(CORES):
            target = chip * CORES + c
            block = mine.at[:, block_of(source * CORES + c)]
            for side in sides:
                send(block, joint, (target, at(a, side)), dst)
            if has_line:
                send(block, line_sem, (target, at(twin, b)), dst)
                send_middle(block, line_sem, (target, at(mirror, b)), dst)
        send(mine.at[:, block_of(source * CORES + 1 - core)], joint, (mate, t), dst)

    own_block(chip, cols_ref.at[chip, core, t], own_line_sem(a), own_joint)
    for n, other in enumerate(chips):
        block = mine.at[:, pair_of(other)]
        for side in sides:
            send(block, extra_joint(n), (dp, at(a, side)), extra.at[n, t])
        if has_line:
            send(block, extra_line_sem(n, a), (dp, at(twin, b)), extra.at[n, t])
            send_middle(block, extra_line_sem(n, a), (dp, at(mirror, b)), extra.at[n, t])

    def own_far():
        @pl.when(middle == 1)
        def _():
            pl.semaphore_wait(ready_sem.at[0], 1)
            pl.semaphore_signal(ready_sem.at[1], inc=1, device_id=(dp, at(twin, b)), device_id_type=MESH)

        @pl.when(middle == 0)
        def _():
            pl.semaphore_wait(ready_sem.at[1], 1)

        for c in range(CORES):
            block = mine.at[:, block_of(chip * CORES + c)]
            send_end(block, own_line_sem(a), (chip * CORES + c, at(mirror, b)), cols_ref.at[chip, core, t])
        for n, other in enumerate(chips):
            send_end(mine.at[:, pair_of(other)], extra_line_sem(n, a), (dp, at(mirror, b)), extra.at[n, t])

    with jax.named_scope("hid_load"):
        loads[1].wait()
        loads[2].wait()
    slices = [
        (plain.at[n], distant.at[n], other * CORES * feats, start, width)
        for n, other in enumerate(chips) for start, width in cut(CORES * feats, SLICE)
    ]
    slices += [(flat, weight, dp * feats, start, width) for start, width in cut(feats, SLICE)]
    n_own = len(cut(feats, SLICE))
    weight_loads = [
        pltpu.make_async_copy(
            weight_hbm.at[:, pl.ds(pl.multiple_of(first + start, width), width)], raw.at[:, pl.ds(start, width)], weight_sem.at[k],
        )
        for k, (raw, _, first, start, width) in enumerate(slices)
    ]
    with jax.named_scope("hid"):
        g = gate[...].astype(jnp.float32)
        u = upper[...].astype(jnp.float32)
        sig = jax.nn.sigmoid(g)
        hidden_ref[chip, core] = (g * sig * u).astype(jnp.bfloat16)
        act_ref[...] = g * sig
        slope_ref[...] = u * sig * (1.0 + g * (1.0 - sig))
    hidden_mate, grad_mate = hidden_sem.at[len(pieces)], hidden_sem.at[len(pieces) + 1]
    for k, (start, width) in enumerate(pieces):
        piece = hidden_ref.at[chip, core, :, pl.ds(start, width)]
        for other in chips:
            copy_to(piece, hidden_sem.at[k], (other * CORES + core, t), lane=1).start()
    copy_to(hidden_ref.at[chip, core], hidden_mate, (mate, t), lane=1).start()
    for load in weight_loads:
        load.start()
    if has_line:
        with jax.named_scope("own_far"):
            own_far()
    cols_ref[chip, core, t] = mine[:, block_of(dp)]
    for n, other in enumerate(chips):
        extra[n, t] = mine[:, pair_of(other)]

    def onward(i):
        return (dp, at(mirror if i == 0 else twin, b))

    def only(job):
        counted = set()

        def run(*args, where=None):
            kept = list(sent), list(sent_middle), list(sent_end)
            if where is None:
                job(*args)
            else:
                pl.when(middle == where)(functools.partial(job, *args))
            if args in counted:
                sent[:], sent_middle[:], sent_end[:] = kept
            counted.add(args)

        return run

    @only
    def own_line(i):
        block, sem = cols_ref.at[chip, :, at(line[i], b)], own_line_sem(line[i])
        arrived(CORES, sem)
        if i < 2:
            send_middle(block, sem, onward(i))
        for side in sides:
            send(block, own_joint, (dp, at(a, side)))

    @only
    def extra_line(i):
        source = at(line[i], b)
        for n, other in enumerate(chips):
            block, sem = extra.at[n, source], extra_line_sem(n, line[i])
            arrived(CORES, sem)
            if i < 2:
                send_middle(block, sem, onward(i))
            for side in sides:
                send(block, extra_joint(n), (dp, at(a, side)))
            if i == 2:
                for c in range(CORES):
                    block = extra.at[n, source, :, pl.ds(c * feats, feats)]
                    for side in [b] + sides:
                        send(block, late, (other * CORES + c, at(a, side)), cols_ref.at[chip, core, source])

    @only
    def own_last():
        arrived(n_side * (1 + n_line) * CORES + 1, own_joint)

    @only
    def extra_last():
        for n in range(n_other):
            arrived(n_side * (1 + n_line) * CORES, extra_joint(n))

    def cols_along(side):
        for other in chips:
            block = cols_ref.at[other, :, at(a, side)]
            send(block, late, (dp, at(twin, b)))
            send_middle(block, late, (dp, at(mirror, b)))
            send_middle(block, late, (dp, at(across, b)))

    @only
    def cols_own():
        arrived(n_other * CORES, cross)
        for other in chips:
            for side in sides:
                send(cols_ref.at[other, :, t], from_sides, (dp, at(a, side)))
        if has_line:
            cols_along(b)

    @only
    def cols_sides():
        if n_side:
            arrived(n_other * n_side * CORES, from_sides)
        if has_line:
            for side in sides:
                cols_along(side)

    def cols_last():
        if has_line:
            arrived(3 * n_other * (1 + n_side) * CORES, late)

    @only
    def hidden_piece(k):
        start, width = pieces[k]
        for other in chips:
            piece = hidden_ref.at[other, core, :, pl.ds(start, width)]
            copy_to(piece, hidden_sem.at[k], (mate, t), lane=1).wait_recv()
        for other in chips:
            piece = hidden_ref.at[other, core, :, pl.ds(start, width)]
            copy_to(piece, hidden_mate, (mate, t), lane=1).start()

    def scoped(name, job, *args):
        with jax.named_scope(name):
            return job(*args)

    def dot(k):
        if k >= len(spans):
            return
        if k == 0:
            for place, owner in enumerate((core, 1 - core)):
                left[pl.ds(place * group, group)] = (
                    cols_ref[chip, owner].astype(jnp.float32).reshape(group, feats).astype(jnp.bfloat16)
                )
        start, width = spans[k]
        span = pl.ds(start, width)
        term = lax.dot_general(
            left[...], weight[:, span], (((1,), (0,)), ((), ())), preferred_element_type=jnp.float32
        )
        grad_ref[:, span] = term[:group]
        leave[:, span] = term[group:].astype(jnp.bfloat16)
        copy_to(leave.at[:, span], grad_mate, (mate, t), other_ref.at[:, span], 1).start()

    def turn(q):
        for k, (raw, turned, _, start, width) in enumerate(slices):
            far = len(slices) - n_own
            if (k * TURNS // far if k < far else TURNS) == q:
                weight_loads[k].wait()
                span = pl.ds(start, width)
                turned[span] = raw[:, span].T

    jobs = {
        "own": own_line, "extra": extra_line, "cols": cols_own, "sides": cols_sides,
        "owns": own_last, "extras": extra_last, "hidden": hidden_piece, "dots": dot, "turn": turn,
    }
    line_jobs = ("own", "extra")
    for name, *rest in ORDER:
        if name in line_jobs and not has_line or name == "hidden" and rest[0] >= len(pieces):
            continue
        where = rest.pop() if rest and rest[-1] in (MIDDLE, END) else None
        if where is None:
            scoped(name + "".join(map(str, rest)), jobs[name], *rest)
        else:
            scoped(name + "".join(map(str, rest)) + where[0], functools.partial(jobs[name], where=int(where == MIDDLE)), *rest)

    with jax.named_scope("tail_cols"):
        cols_last()
    with jax.named_scope("tail_hid"):
        everyone = hidden_ref.at[:, 1 - core]
        copy_to(everyone, hidden_mate, (mate, t), lane=1).wait_recv()
    with jax.named_scope("tail_grad"):
        copy_to(leave, grad_mate, (mate, t), other_ref, 1).wait_recv()
    with jax.named_scope("tail_send"):
        copy_to(gauge.at[pl.ds(0, sum(sent))], late, (mate, t)).wait_send()
        if has_line:

            @pl.when(middle == 1)
            def _():
                copy_to(gauge.at[pl.ds(0, sum(sent_middle))], late, (mate, t)).wait_send()

            @pl.when(middle == 0)
            def _():
                copy_to(gauge.at[pl.ds(0, sum(sent_end))], late, (mate, t)).wait_send()

        copy_to(hidden_ref, hidden_mate, (mate, t), lane=1).wait_send()


def finish_kernel(
    spans, chunks, cols_ref, hidden_ref, grad_ref, other_ref, act_ref, slope_ref, extra_ref, distant_ref,
    weight_out, gate_out, up_out, turned, gate, upper, left, weight_sem, grad_sem,
):
    copies = []

    def leave(src, dst, sem):
        copies.append(pltpu.make_async_copy(src, dst, sem))
        copies[-1].start()

    for k, (start, width) in enumerate(spans):
        span = pl.ds(start, width)
        turned[span] = lax.dot_general(
            hidden_ref[:, span], cols_ref[...], (((0,), (0,)), ((), ())), preferred_element_type=jnp.float32
        )
        leave(turned.at[span], weight_out.at[span], weight_sem.at[k])
    n_other, _, _, pair = extra_ref.shape
    for n in range(n_other):
        left[n] = extra_ref[n].astype(jnp.float32).reshape(left.shape[1], pair).astype(jnp.bfloat16)
    for k, (start, width) in enumerate(chunks):
        span = pl.ds(start, width)
        grad = grad_ref[:, span] + other_ref[:, span].astype(jnp.float32)
        for n in range(n_other):
            grad += jnp.dot(left[n], distant_ref[n, :, span], preferred_element_type=jnp.float32)
        upper[:, span] = (grad * act_ref[:, span]).astype(jnp.bfloat16)
        gate[:, span] = (grad * slope_ref[:, span]).astype(jnp.bfloat16)
    leave(upper, up_out, grad_sem.at[0])
    leave(gate, gate_out, grad_sem.at[1])
    for copy in copies:
        copy.wait()


def body(n_dp, n_t, grad_out, gate_pre, up_pre, down_weight):
    depth, model = grad_out.shape
    group, wide = gate_pre.shape
    feats = model // n_dp
    n_chip = n_dp // CORES
    outer = 4 if n_t % 4 == 0 else 1
    inner = n_t // outer
    spans = cut(wide, 1024)
    pieces = cut(wide, 1024)
    n_side, n_other = inner - 1, n_chip - 1
    n_gauge = (n_chip + 1) * (n_side + 4) * 2 + 3 * n_side * 2 + n_other * (16 * n_side + 12)
    lanes = pl.cdiv(wide, 128) * 128
    pair = CORES * feats
    results = 2 * (n_dp * group * (feats + lanes) + 7 * group * lanes + n_other * (group + lanes) * pair)
    limit = VMEM - results - 64 * 1024
    anywhere = pl.BlockSpec(memory_space=pltpu.HBM)
    vmem = pl.BlockSpec(memory_space=pltpu.VMEM)
    dma = pltpu.SemaphoreType.DMA
    cols, hidden, *factors = pl.pallas_call(
        functools.partial(gather_kernel, n_dp, n_t, outer, spans, pieces),
        out_shape=[
            pltpu.VMEM((n_chip, CORES, n_t, depth, feats), jnp.bfloat16),
            pltpu.VMEM((n_chip, CORES, group, wide), jnp.bfloat16),
            pltpu.VMEM((group, wide), jnp.float32),
            pltpu.VMEM((group, wide), jnp.bfloat16),
            pltpu.VMEM((group, wide), jnp.float32),
            pltpu.VMEM((group, wide), jnp.float32),
            pltpu.VMEM((n_other, n_t, depth, pair), jnp.bfloat16),
            pltpu.VMEM((n_other, pair, wide), jnp.bfloat16),
        ],
        in_specs=[anywhere] * 4,
        out_specs=[vmem] * 8,
        scratch_shapes=[
            pltpu.VMEM((depth, model), jnp.bfloat16),
            pltpu.VMEM((group, wide), jnp.bfloat16),
            pltpu.VMEM((group, wide), jnp.bfloat16),
            pltpu.VMEM((feats, wide), jnp.bfloat16),
            pltpu.VMEM((wide, feats), jnp.bfloat16),
            pltpu.VMEM((n_other, wide, pair), jnp.bfloat16),
            pltpu.VMEM((CORES * group, feats), jnp.bfloat16),
            pltpu.VMEM((group, wide), jnp.bfloat16),
            pltpu.VMEM((n_gauge, depth, feats), jnp.bfloat16),
            dma((3,)),
            dma((n_other * len(cut(pair, SLICE)) + len(cut(feats, SLICE)),)),
            dma((2,)),
            pltpu.SemaphoreType.REGULAR((2,)),
            dma((outer + 1,)),
            dma((n_other, outer + 1)),
            dma((3,)),
            dma((len(pieces) + 2,)),
        ],
        compiler_params=pltpu.CompilerParams(collective_id=0, has_side_effects=True, vmem_limit_bytes=limit),
    )(grad_out, gate_pre, up_pre, down_weight.T)
    cols = cols.reshape(n_dp * group, feats)
    hidden = hidden.reshape(n_dp * group, wide)

    steps = [(0, min(128, wide))] + [(128 + start, width) for start, width in cut(wide - 128, 256)]
    turned, grad_gate, grad_up = pl.pallas_call(
        functools.partial(finish_kernel, steps, cut(wide, 512)),
        out_shape=[
            jax.ShapeDtypeStruct((wide, feats), jnp.float32),
            jax.ShapeDtypeStruct((group, wide), jnp.bfloat16),
            jax.ShapeDtypeStruct((group, wide), jnp.bfloat16),
        ],
        in_specs=[vmem] * 8,
        out_specs=[anywhere] * 3,
        scratch_shapes=[
            pltpu.VMEM((wide, feats), jnp.float32),
            pltpu.VMEM((group, wide), jnp.bfloat16),
            pltpu.VMEM((group, wide), jnp.bfloat16),
            pltpu.VMEM((n_other, group, pair), jnp.bfloat16),
            dma((len(steps),)),
            dma((2,)),
        ],
        compiler_params=pltpu.CompilerParams(vmem_limit_bytes=limit),
    )(*[pltpu.with_memory_space_constraint(x, pltpu.VMEM) for x in (cols, hidden, *factors)])
    return turned.T, grad_gate, grad_up


def solution(mesh):
    in_specs = (P(("dp", "tensor"), None), P("dp", "tensor"), P("dp", "tensor"), P(None, "tensor"))
    out_specs = (P("dp", "tensor"), P("dp", "tensor"), P("dp", "tensor"))
    fn = functools.partial(body, mesh.shape["dp"], mesh.shape["tensor"])
    return jax.shard_map(fn, mesh=mesh, in_specs=in_specs, out_specs=out_specs, check_vma=False)
```

```python
import functools

import jax
import jax.numpy as jnp
from jax import lax
from jax.experimental import pallas as pl
from jax.experimental.pallas import tpu as pltpu
from jax.sharding import PartitionSpec as P

MESH = pl.DeviceIdType.MESH
CORES = 2
VMEM = 67043328
SLICE = 512
TURNS = 4
MIDDLE, END = "middle", "end"
ORDER = (
    ("own", 0),
    ("own", 1, MIDDLE),
    ("cols",),
    ("extra", 0),
    ("extra", 1, MIDDLE),
    ("turn", 0),
    ("turn", 1),
    ("own", 1, END),
    ("own", 2),
    ("turn", 2),
    ("turn", 3),
    ("extra", 1, END),
    ("sides",),
    ("extra", 2),
    ("far",),
    ("turn", 4),
    ("hidden", 0),
    ("owns",),
    ("dots", 0),
    ("hidden", 1),
    ("dots", 1),
    ("extras",),
)


def cut(wide, step):
    return [(start, min(step, wide - start)) for start in range(0, wide, step)]


def gather_kernel(
    n_dp, n_t, outer, spans, pieces,
    go_hbm, gate_hbm, up_hbm, weight_hbm,
    cols_ref, hidden_ref, grad_ref, other_ref, act_ref, slope_ref, extra, distant,
    mine, gate, upper, weight, flat, plain, left, leave, gauge,
    load_sem, weight_sem, send_sem, ready_sem, own_sem, extra_sem, cols_sem, hidden_sem,
):
    inner = n_t // outer
    n_chip = n_dp // CORES
    depth, feats = mine.shape[0], cols_ref.shape[-1]
    group = n_t * depth
    dp, t = lax.axis_index("dp"), lax.axis_index("tensor")
    chip, core = dp // CORES, dp % CORES
    mate = chip * CORES + (1 - core)
    a, b = t // inner, t % inner
    chips = [lax.rem(chip + d, n_chip) for d in range(1, n_chip)]
    sides = [lax.rem(b + d, inner) for d in range(1, inner)]
    n_other, n_side = len(chips), len(sides)

    has_line = outer == 4
    middle = (a * (3 - a)) // 2
    twin, mirror, across = a + 1 - 2 * (a % 2), 3 - a, (a + 2) % 4
    second = middle * mirror + (1 - middle) * across
    third = middle * across + (1 - middle) * mirror
    line = [twin, second, third] if has_line else []
    n_line = len(line)

    own_joint = own_sem.at[outer]
    cross, from_sides, late = (cols_sem.at[k] for k in range(3))

    def own_line_sem(step):
        return own_sem.at[step]

    def extra_line_sem(other, step):
        return extra_sem.at[other, step]

    def extra_joint(other):
        return extra_sem.at[other, outer]

    def at(step, side):
        return step * inner + side

    loads = [
        pltpu.make_async_copy(go_hbm, mine, load_sem.at[0]),
        pltpu.make_async_copy(gate_hbm, gate, load_sem.at[1]),
        pltpu.make_async_copy(up_hbm, upper, load_sem.at[2]),
    ]
    for load in loads:
        load.start()

    barrier = pltpu.get_barrier_semaphore()
    peers = [(lax.rem(dp + d, n_dp), t) for d in range(1, n_dp)]
    for c in range(CORES):
        peers += [(chip * CORES + c, at(a, side)) for side in sides]
        if has_line:
            peers.append((chip * CORES + c, at(twin, b)))
    for peer in peers:
        pl.semaphore_signal(barrier, inc=1, device_id=peer, device_id_type=MESH)
    if has_line:

        @pl.when(middle == 1)
        def _():
            for c in range(CORES):
                pl.semaphore_signal(barrier, inc=1, device_id=(chip * CORES + c, at(mirror, b)), device_id_type=MESH)

    with jax.named_scope("go"):
        loads[0].wait()
    with jax.named_scope("barrier"):
        pl.semaphore_wait(barrier, len(peers) + (CORES * middle if has_line else 0))

    if has_line:

        @pl.when(middle == 1)
        def _():
            pl.semaphore_signal(ready_sem.at[0], inc=1, device_id=(dp, at(mirror, b)), device_id_type=MESH)

    sent, sent_middle, sent_end = [], [], []

    def copy_to(block, sem, peer, dst=None, lane=0):
        return pltpu.make_async_remote_copy(
            src_ref=block, dst_ref=block if dst is None else dst, send_sem=send_sem.at[lane], recv_sem=sem,
            device_id=peer, device_id_type=MESH,
        )

    def arrived(blocks, sem):
        copy_to(gauge.at[pl.ds(0, blocks)], sem, (mate, t)).wait_recv()

    def block_of(group):
        return pl.ds(pl.multiple_of(group * feats, feats), feats)

    def blocks_in(block):
        size = 1
        for dim in block.shape:
            size *= dim
        return size // (depth * feats)

    def send(block, sem, peer, dst=None):
        sent.append(blocks_in(block))
        copy_to(block, sem, peer, dst).start()

    def send_middle(block, sem, peer, dst=None):
        sent_middle.append(blocks_in(block))

        @pl.when(middle == 1)
        def _():
            copy_to(block, sem, peer, dst).start()

    for other in chips:
        for c in range(CORES):
            group_of = other * CORES + c
            send(mine.at[:, block_of(group_of)], cross, (group_of, t), cols_ref.at[chip, core, t])

    def send_end(block, sem, peer, dst=None):
        sent_end.append(blocks_in(block))

        @pl.when(middle == 0)
        def _():
            copy_to(block, sem, peer, dst).start()

    def pair_of(other):
        return pl.ds(pl.multiple_of(other * CORES * feats, CORES * feats), CORES * feats)

    def own_block(source, dst, line_sem, joint):
        for c in range(CORES):
            target = chip * CORES + c
            block = mine.at[:, block_of(source * CORES + c)]
            for side in sides:
                send(block, joint, (target, at(a, side)), dst)
            if has_line:
                send(block, line_sem, (target, at(twin, b)), dst)
                send_middle(block, line_sem, (target, at(mirror, b)), dst)
        send(mine.at[:, block_of(source * CORES + 1 - core)], joint, (mate, t), dst)

    own_block(chip, cols_ref.at[chip, core, t], own_line_sem(a), own_joint)
    for n, other in enumerate(chips):
        block = mine.at[:, pair_of(other)]
        for side in sides:
            send(block, extra_joint(n), (dp, at(a, side)), extra.at[n, t])
        if has_line:
            send(block, extra_line_sem(n, a), (dp, at(twin, b)), extra.at[n, t])
            send_middle(block, extra_line_sem(n, a), (dp, at(mirror, b)), extra.at[n, t])

    def own_far():
        @pl.when(middle == 1)
        def _():
            pl.semaphore_wait(ready_sem.at[0], 1)
            pl.semaphore_signal(ready_sem.at[1], inc=1, device_id=(dp, at(twin, b)), device_id_type=MESH)

        @pl.when(middle == 0)
        def _():
            pl.semaphore_wait(ready_sem.at[1], 1)

        for c in range(CORES):
            block = mine.at[:, block_of(chip * CORES + c)]
            send_end(block, own_line_sem(a), (chip * CORES + c, at(mirror, b)), cols_ref.at[chip, core, t])
            send_middle(block, own_line_sem(a), (chip * CORES + c, at(across, b)), cols_ref.at[chip, core, t])
        for n, other in enumerate(chips):
            block = mine.at[:, pair_of(other)]
            send_end(block, extra_line_sem(n, a), (dp, at(mirror, b)), extra.at[n, t])
            send_middle(block, extra_line_sem(n, a), (dp, at(across, b)), extra.at[n, t])

    with jax.named_scope("hid_load"):
        loads[1].wait()
        loads[2].wait()
    slices = [
        (plain.at[n], distant.at[n], other * CORES * feats, start, width)
        for n, other in enumerate(chips) for start, width in cut(CORES * feats, SLICE)
    ]
    slices += [(flat, weight, dp * feats, start, width) for start, width in cut(feats, SLICE)]
    n_own = len(cut(feats, SLICE))
    weight_loads = [
        pltpu.make_async_copy(
            weight_hbm.at[:, pl.ds(pl.multiple_of(first + start, width), width)], raw.at[:, pl.ds(start, width)], weight_sem.at[k],
        )
        for k, (raw, _, first, start, width) in enumerate(slices)
    ]
    with jax.named_scope("hid"):
        g = gate[...].astype(jnp.float32)
        u = upper[...].astype(jnp.float32)
        sig = jax.nn.sigmoid(g)
        hidden_ref[chip, core] = (g * sig * u).astype(jnp.bfloat16)
        act_ref[...] = g * sig
        slope_ref[...] = u * sig * (1.0 + g * (1.0 - sig))
    hidden_mate, grad_mate = hidden_sem.at[len(pieces)], hidden_sem.at[len(pieces) + 1]
    for k, (start, width) in enumerate(pieces):
        piece = hidden_ref.at[chip, core, :, pl.ds(start, width)]
        for other in chips:
            copy_to(piece, hidden_sem.at[k], (other * CORES + core, t), lane=1).start()
    copy_to(hidden_ref.at[chip, core], hidden_mate, (mate, t), lane=1).start()
    for load in weight_loads:
        load.start()
    if has_line:
        with jax.named_scope("own_far"):
            own_far()
    cols_ref[chip, core, t] = mine[:, block_of(dp)]
    for n, other in enumerate(chips):
        extra[n, t] = mine[:, pair_of(other)]

    def only(job):
        counted = set()

        def run(*args, where=None):
            kept = list(sent), list(sent_middle), list(sent_end)
            if where is None:
                job(*args)
            else:
                pl.when(middle == where)(functools.partial(job, *args))
            if args in counted:
                sent[:], sent_middle[:], sent_end[:] = kept
            counted.add(args)

        return run

    @only
    def own_line(i):
        block, sem = cols_ref.at[chip, :, at(line[i], b)], own_line_sem(line[i])
        arrived(CORES, sem)
        if i == 0:
            send_middle(block, sem, (dp, at(mirror, b)))
        for side in sides:
            send(block, own_joint, (dp, at(a, side)))

    @only
    def extra_line(i):
        source = at(line[i], b)
        for n, other in enumerate(chips):
            block, sem = extra.at[n, source], extra_line_sem(n, line[i])
            arrived(CORES, sem)
            if i == 0:
                send_middle(block, sem, (dp, at(mirror, b)))
            for side in sides:
                send(block, extra_joint(n), (dp, at(a, side)))

    def extra_far():
        source = at(third, b)
        for n, other in enumerate(chips):
            for c in range(CORES):
                block = extra.at[n, source, :, pl.ds(c * feats, feats)]
                for side in [b] + sides:
                    send(block, late, (other * CORES + c, at(a, side)), cols_ref.at[chip, core, source])

    @only
    def own_last():
        arrived(n_side * (1 + n_line) * CORES + 1, own_joint)

    @only
    def extra_last():
        for n in range(n_other):
            arrived(n_side * (1 + n_line) * CORES, extra_joint(n))

    def cols_along(side):
        for other in chips:
            block = cols_ref.at[other, :, at(a, side)]
            send(block, late, (dp, at(twin, b)))
            send_middle(block, late, (dp, at(mirror, b)))
            send_middle(block, late, (dp, at(across, b)))

    @only
    def cols_own():
        arrived(n_other * CORES, cross)
        for other in chips:
            for side in sides:
                send(cols_ref.at[other, :, t], from_sides, (dp, at(a, side)))
        if has_line:
            cols_along(b)

    @only
    def cols_sides():
        if n_side:
            arrived(n_other * n_side * CORES, from_sides)
        if has_line:
            for side in sides:
                cols_along(side)

    def cols_last():
        if has_line:
            arrived(3 * n_other * (1 + n_side) * CORES, late)

    @only
    def hidden_piece(k):
        start, width = pieces[k]
        for other in chips:
            piece = hidden_ref.at[other, core, :, pl.ds(start, width)]
            copy_to(piece, hidden_sem.at[k], (mate, t), lane=1).wait_recv()
        for other in chips:
            piece = hidden_ref.at[other, core, :, pl.ds(start, width)]
            copy_to(piece, hidden_mate, (mate, t), lane=1).start()

    def scoped(name, job, *args):
        with jax.named_scope(name):
            return job(*args)

    def dot(k):
        if k >= len(spans):
            return
        if k == 0:
            for place, owner in enumerate((core, 1 - core)):
                left[pl.ds(place * group, group)] = (
                    cols_ref[chip, owner].astype(jnp.float32).reshape(group, feats).astype(jnp.bfloat16)
                )
        start, width = spans[k]
        span = pl.ds(start, width)
        term = lax.dot_general(
            left[...], weight[:, span], (((1,), (0,)), ((), ())), preferred_element_type=jnp.float32
        )
        grad_ref[:, span] = term[:group]
        leave[:, span] = term[group:].astype(jnp.bfloat16)
        copy_to(leave.at[:, span], grad_mate, (mate, t), other_ref.at[:, span], 1).start()

    def turn(q):
        for k, (raw, turned, _, start, width) in enumerate(slices):
            far = len(slices) - n_own
            if (k * TURNS // far if k < far else TURNS) == q:
                weight_loads[k].wait()
                span = pl.ds(start, width)
                turned[span] = raw[:, span].T

    jobs = {
        "own": own_line, "extra": extra_line, "cols": cols_own, "sides": cols_sides,
        "owns": own_last, "extras": extra_last, "hidden": hidden_piece, "dots": dot, "turn": turn, "far": extra_far,
    }
    line_jobs = ("own", "extra", "far")
    for name, *rest in ORDER:
        if name in line_jobs and not has_line or name == "hidden" and rest[0] >= len(pieces):
            continue
        where = rest.pop() if rest and rest[-1] in (MIDDLE, END) else None
        if where is None:
            scoped(name + "".join(map(str, rest)), jobs[name], *rest)
        else:
            scoped(name + "".join(map(str, rest)) + where[0], functools.partial(jobs[name], where=int(where == MIDDLE)), *rest)

    with jax.named_scope("tail_cols"):
        cols_last()
    with jax.named_scope("tail_hid"):
        everyone = hidden_ref.at[:, 1 - core]
        copy_to(everyone, hidden_mate, (mate, t), lane=1).wait_recv()
    with jax.named_scope("tail_grad"):
        copy_to(leave, grad_mate, (mate, t), other_ref, 1).wait_recv()
    with jax.named_scope("tail_send"):
        copy_to(gauge.at[pl.ds(0, sum(sent))], late, (mate, t)).wait_send()
        if has_line:

            @pl.when(middle == 1)
            def _():
                copy_to(gauge.at[pl.ds(0, sum(sent_middle))], late, (mate, t)).wait_send()

            @pl.when(middle == 0)
            def _():
                copy_to(gauge.at[pl.ds(0, sum(sent_end))], late, (mate, t)).wait_send()

        copy_to(hidden_ref, hidden_mate, (mate, t), lane=1).wait_send()


def finish_kernel(
    spans, chunks, cols_ref, hidden_ref, grad_ref, other_ref, act_ref, slope_ref, extra_ref, distant_ref,
    weight_out, gate_out, up_out, turned, gate, upper, left, weight_sem, grad_sem,
):
    copies = []

    def leave(src, dst, sem):
        copies.append(pltpu.make_async_copy(src, dst, sem))
        copies[-1].start()

    for k, (start, width) in enumerate(spans):
        span = pl.ds(start, width)
        turned[span] = lax.dot_general(
            hidden_ref[:, span], cols_ref[...], (((0,), (0,)), ((), ())), preferred_element_type=jnp.float32
        )
        leave(turned.at[span], weight_out.at[span], weight_sem.at[k])
    n_other, _, _, pair = extra_ref.shape
    for n in range(n_other):
        left[n] = extra_ref[n].astype(jnp.float32).reshape(left.shape[1], pair).astype(jnp.bfloat16)
    for k, (start, width) in enumerate(chunks):
        span = pl.ds(start, width)
        grad = grad_ref[:, span] + other_ref[:, span].astype(jnp.float32)
        for n in range(n_other):
            grad += jnp.dot(left[n], distant_ref[n, :, span], preferred_element_type=jnp.float32)
        upper[:, span] = (grad * act_ref[:, span]).astype(jnp.bfloat16)
        gate[:, span] = (grad * slope_ref[:, span]).astype(jnp.bfloat16)
    leave(upper, up_out, grad_sem.at[0])
    leave(gate, gate_out, grad_sem.at[1])
    for copy in copies:
        copy.wait()


def body(n_dp, n_t, grad_out, gate_pre, up_pre, down_weight):
    depth, model = grad_out.shape
    group, wide = gate_pre.shape
    feats = model // n_dp
    n_chip = n_dp // CORES
    outer = 4 if n_t % 4 == 0 else 1
    inner = n_t // outer
    spans = cut(wide, 1024)
    pieces = cut(wide, 1024)
    n_side, n_other = inner - 1, n_chip - 1
    n_gauge = (n_chip + 1) * (n_side + 4) * 2 + 3 * n_side * 2 + n_other * (16 * n_side + 12)
    lanes = pl.cdiv(wide, 128) * 128
    pair = CORES * feats
    results = 2 * (n_dp * group * (feats + lanes) + 7 * group * lanes + n_other * (group + lanes) * pair)
    limit = VMEM - results - 64 * 1024
    anywhere = pl.BlockSpec(memory_space=pltpu.HBM)
    vmem = pl.BlockSpec(memory_space=pltpu.VMEM)
    dma = pltpu.SemaphoreType.DMA
    cols, hidden, *factors = pl.pallas_call(
        functools.partial(gather_kernel, n_dp, n_t, outer, spans, pieces),
        out_shape=[
            pltpu.VMEM((n_chip, CORES, n_t, depth, feats), jnp.bfloat16),
            pltpu.VMEM((n_chip, CORES, group, wide), jnp.bfloat16),
            pltpu.VMEM((group, wide), jnp.float32),
            pltpu.VMEM((group, wide), jnp.bfloat16),
            pltpu.VMEM((group, wide), jnp.float32),
            pltpu.VMEM((group, wide), jnp.float32),
            pltpu.VMEM((n_other, n_t, depth, pair), jnp.bfloat16),
            pltpu.VMEM((n_other, pair, wide), jnp.bfloat16),
        ],
        in_specs=[anywhere] * 4,
        out_specs=[vmem] * 8,
        scratch_shapes=[
            pltpu.VMEM((depth, model), jnp.bfloat16),
            pltpu.VMEM((group, wide), jnp.bfloat16),
            pltpu.VMEM((group, wide), jnp.bfloat16),
            pltpu.VMEM((feats, wide), jnp.bfloat16),
            pltpu.VMEM((wide, feats), jnp.bfloat16),
            pltpu.VMEM((n_other, wide, pair), jnp.bfloat16),
            pltpu.VMEM((CORES * group, feats), jnp.bfloat16),
            pltpu.VMEM((group, wide), jnp.bfloat16),
            pltpu.VMEM((n_gauge, depth, feats), jnp.bfloat16),
            dma((3,)),
            dma((n_other * len(cut(pair, SLICE)) + len(cut(feats, SLICE)),)),
            dma((2,)),
            pltpu.SemaphoreType.REGULAR((2,)),
            dma((outer + 1,)),
            dma((n_other, outer + 1)),
            dma((3,)),
            dma((len(pieces) + 2,)),
        ],
        compiler_params=pltpu.CompilerParams(collective_id=0, has_side_effects=True, vmem_limit_bytes=limit),
    )(grad_out, gate_pre, up_pre, down_weight.T)
    cols = cols.reshape(n_dp * group, feats)
    hidden = hidden.reshape(n_dp * group, wide)

    steps = [(0, min(128, wide))] + [(128 + start, width) for start, width in cut(wide - 128, 256)]
    turned, grad_gate, grad_up = pl.pallas_call(
        functools.partial(finish_kernel, steps, cut(wide, 512)),
        out_shape=[
            jax.ShapeDtypeStruct((wide, feats), jnp.float32),
            jax.ShapeDtypeStruct((group, wide), jnp.bfloat16),
            jax.ShapeDtypeStruct((group, wide), jnp.bfloat16),
        ],
        in_specs=[vmem] * 8,
        out_specs=[anywhere] * 3,
        scratch_shapes=[
            pltpu.VMEM((wide, feats), jnp.float32),
            pltpu.VMEM((group, wide), jnp.bfloat16),
            pltpu.VMEM((group, wide), jnp.bfloat16),
            pltpu.VMEM((n_other, group, pair), jnp.bfloat16),
            dma((len(steps),)),
            dma((2,)),
        ],
        compiler_params=pltpu.CompilerParams(vmem_limit_bytes=limit),
    )(*[pltpu.with_memory_space_constraint(x, pltpu.VMEM) for x in (cols, hidden, *factors)])
    return turned.T, grad_gate, grad_up


def solution(mesh):
    in_specs = (P(("dp", "tensor"), None), P("dp", "tensor"), P("dp", "tensor"), P(None, "tensor"))
    out_specs = (P("dp", "tensor"), P("dp", "tensor"), P("dp", "tensor"))
    fn = functools.partial(body, mesh.shape["dp"], mesh.shape["tensor"])
    return jax.shard_map(fn, mesh=mesh, in_specs=in_specs, out_specs=out_specs, check_vma=False)
```

```python
import functools

import jax
import jax.numpy as jnp
from jax import lax
from jax.experimental import pallas as pl
from jax.experimental.pallas import tpu as pltpu
from jax.sharding import PartitionSpec as P

MESH = pl.DeviceIdType.MESH
CORES = 2
VMEM = 67043328
SLICE = 512
TURNS = 4
MIDDLE, END = "middle", "end"
ORDER = (
    ("own", 0),
    ("own", 1, MIDDLE),
    ("cols",),
    ("extra", 0),
    ("extra", 1, MIDDLE),
    ("turn", 0),
    ("turn", 1),
    ("own", 1, END),
    ("own", 2),
    ("sides",),
    ("extra", 1, END),
    ("extra", 2),
    ("far",),
    ("turn", 4),
    ("hidden", 0),
    ("owns",),
    ("dots", 0),
    ("hidden", 1),
    ("dots", 1),
    ("turn", 2),
    ("turn", 3),
    ("extras",),
)


def cut(wide, step):
    return [(start, min(step, wide - start)) for start in range(0, wide, step)]


def gather_kernel(
    n_dp, n_t, outer, spans, pieces,
    go_hbm, gate_hbm, up_hbm, weight_hbm,
    cols_ref, hidden_ref, grad_ref, other_ref, act_ref, slope_ref, extra, distant,
    mine, gate, upper, weight, flat, plain, left, leave, gauge,
    load_sem, weight_sem, send_sem, ready_sem, own_sem, extra_sem, cols_sem, hidden_sem,
):
    inner = n_t // outer
    n_chip = n_dp // CORES
    depth, feats = mine.shape[0], cols_ref.shape[-1]
    group = n_t * depth
    dp, t = lax.axis_index("dp"), lax.axis_index("tensor")
    chip, core = dp // CORES, dp % CORES
    mate = chip * CORES + (1 - core)
    a, b = t // inner, t % inner
    chips = [lax.rem(chip + d, n_chip) for d in range(1, n_chip)]
    sides = [lax.rem(b + d, inner) for d in range(1, inner)]
    n_other, n_side = len(chips), len(sides)

    has_line = outer == 4
    middle = (a * (3 - a)) // 2
    twin, mirror, across = a + 1 - 2 * (a % 2), 3 - a, (a + 2) % 4
    second = middle * mirror + (1 - middle) * across
    third = middle * across + (1 - middle) * mirror
    line = [twin, second, third] if has_line else []
    n_line = len(line)

    own_joint = own_sem.at[outer]
    cross, from_sides, late = (cols_sem.at[k] for k in range(3))

    def own_line_sem(step):
        return own_sem.at[step]

    def extra_line_sem(other, step):
        return extra_sem.at[other, step]

    def extra_joint(other):
        return extra_sem.at[other, outer]

    def at(step, side):
        return step * inner + side

    loads = [
        pltpu.make_async_copy(go_hbm, mine, load_sem.at[0]),
        pltpu.make_async_copy(gate_hbm, gate, load_sem.at[1]),
        pltpu.make_async_copy(up_hbm, upper, load_sem.at[2]),
    ]
    for load in loads:
        load.start()

    barrier = pltpu.get_barrier_semaphore()
    peers = [(lax.rem(dp + d, n_dp), t) for d in range(1, n_dp)]
    for c in range(CORES):
        peers += [(chip * CORES + c, at(a, side)) for side in sides]
        if has_line:
            peers.append((chip * CORES + c, at(twin, b)))
    for peer in peers:
        pl.semaphore_signal(barrier, inc=1, device_id=peer, device_id_type=MESH)
    if has_line:

        @pl.when(middle == 1)
        def _():
            for c in range(CORES):
                pl.semaphore_signal(barrier, inc=1, device_id=(chip * CORES + c, at(mirror, b)), device_id_type=MESH)

    with jax.named_scope("go"):
        loads[0].wait()
    with jax.named_scope("barrier"):
        pl.semaphore_wait(barrier, len(peers) + (CORES * middle if has_line else 0))

    if has_line:

        @pl.when(middle == 1)
        def _():
            pl.semaphore_signal(ready_sem.at[0], inc=1, device_id=(dp, at(mirror, b)), device_id_type=MESH)

    sent, sent_middle, sent_end = [], [], []

    def copy_to(block, sem, peer, dst=None, lane=0):
        return pltpu.make_async_remote_copy(
            src_ref=block, dst_ref=block if dst is None else dst, send_sem=send_sem.at[lane], recv_sem=sem,
            device_id=peer, device_id_type=MESH,
        )

    def arrived(blocks, sem):
        copy_to(gauge.at[pl.ds(0, blocks)], sem, (mate, t)).wait_recv()

    def block_of(group):
        return pl.ds(pl.multiple_of(group * feats, feats), feats)

    def blocks_in(block):
        size = 1
        for dim in block.shape:
            size *= dim
        return size // (depth * feats)

    def send(block, sem, peer, dst=None):
        sent.append(blocks_in(block))
        copy_to(block, sem, peer, dst).start()

    def send_middle(block, sem, peer, dst=None):
        sent_middle.append(blocks_in(block))

        @pl.when(middle == 1)
        def _():
            copy_to(block, sem, peer, dst).start()

    for other in chips:
        for c in range(CORES):
            group_of = other * CORES + c
            send(mine.at[:, block_of(group_of)], cross, (group_of, t), cols_ref.at[chip, core, t])

    def send_end(block, sem, peer, dst=None):
        sent_end.append(blocks_in(block))

        @pl.when(middle == 0)
        def _():
            copy_to(block, sem, peer, dst).start()

    def pair_of(other):
        return pl.ds(pl.multiple_of(other * CORES * feats, CORES * feats), CORES * feats)

    def own_block(source, dst, line_sem, joint):
        for c in range(CORES):
            target = chip * CORES + c
            block = mine.at[:, block_of(source * CORES + c)]
            for side in sides:
                send(block, joint, (target, at(a, side)), dst)
            if has_line:
                send(block, line_sem, (target, at(twin, b)), dst)
                send_middle(block, line_sem, (target, at(mirror, b)), dst)
        send(mine.at[:, block_of(source * CORES + 1 - core)], joint, (mate, t), dst)

    own_block(chip, cols_ref.at[chip, core, t], own_line_sem(a), own_joint)
    for n, other in enumerate(chips):
        block = mine.at[:, pair_of(other)]
        for side in sides:
            send(block, extra_joint(n), (dp, at(a, side)), extra.at[n, t])
        if has_line:
            send(block, extra_line_sem(n, a), (dp, at(twin, b)), extra.at[n, t])
            send_middle(block, extra_line_sem(n, a), (dp, at(mirror, b)), extra.at[n, t])

    def own_far():
        @pl.when(middle == 1)
        def _():
            pl.semaphore_wait(ready_sem.at[0], 1)
            pl.semaphore_signal(ready_sem.at[1], inc=1, device_id=(dp, at(twin, b)), device_id_type=MESH)

        @pl.when(middle == 0)
        def _():
            pl.semaphore_wait(ready_sem.at[1], 1)

        for c in range(CORES):
            block = mine.at[:, block_of(chip * CORES + c)]
            send_end(block, own_line_sem(a), (chip * CORES + c, at(mirror, b)), cols_ref.at[chip, core, t])
            send_middle(block, own_line_sem(a), (chip * CORES + c, at(across, b)), cols_ref.at[chip, core, t])
        for n, other in enumerate(chips):
            block = mine.at[:, pair_of(other)]
            send_end(block, extra_line_sem(n, a), (dp, at(mirror, b)), extra.at[n, t])
            send_middle(block, extra_line_sem(n, a), (dp, at(across, b)), extra.at[n, t])

    with jax.named_scope("hid_load"):
        loads[1].wait()
        loads[2].wait()
    slices = [
        (plain.at[n], distant.at[n], other * CORES * feats, start, width)
        for n, other in enumerate(chips) for start, width in cut(CORES * feats, SLICE)
    ]
    slices += [(flat, weight, dp * feats, start, width) for start, width in cut(feats, SLICE)]
    n_own = len(cut(feats, SLICE))
    weight_loads = [
        pltpu.make_async_copy(
            weight_hbm.at[:, pl.ds(pl.multiple_of(first + start, width), width)], raw.at[:, pl.ds(start, width)], weight_sem.at[k],
        )
        for k, (raw, _, first, start, width) in enumerate(slices)
    ]
    with jax.named_scope("hid"):
        g = gate[...].astype(jnp.float32)
        u = upper[...].astype(jnp.float32)
        sig = jax.nn.sigmoid(g)
        hidden_ref[chip, core] = (g * sig * u).astype(jnp.bfloat16)
        act_ref[...] = g * sig
        slope_ref[...] = u * sig * (1.0 + g * (1.0 - sig))
    hidden_mate, grad_mate = hidden_sem.at[len(pieces)], hidden_sem.at[len(pieces) + 1]
    for k, (start, width) in enumerate(pieces):
        piece = hidden_ref.at[chip, core, :, pl.ds(start, width)]
        for other in chips:
            copy_to(piece, hidden_sem.at[k], (other * CORES + core, t), lane=1).start()
    copy_to(hidden_ref.at[chip, core], hidden_mate, (mate, t), lane=1).start()
    for load in weight_loads:
        load.start()
    if has_line:
        with jax.named_scope("own_far"):
            own_far()
    cols_ref[chip, core, t] = mine[:, block_of(dp)]
    for n, other in enumerate(chips):
        extra[n, t] = mine[:, pair_of(other)]

    def only(job):
        counted = set()

        def run(*args, where=None):
            kept = list(sent), list(sent_middle), list(sent_end)
            if where is None:
                job(*args)
            else:
                pl.when(middle == where)(functools.partial(job, *args))
            if args in counted:
                sent[:], sent_middle[:], sent_end[:] = kept
            counted.add(args)

        return run

    @only
    def own_line(i):
        block, sem = cols_ref.at[chip, :, at(line[i], b)], own_line_sem(line[i])
        arrived(CORES, sem)
        if i == 0:
            send_middle(block, sem, (dp, at(mirror, b)))
        for side in sides:
            send(block, own_joint, (dp, at(a, side)))

    @only
    def extra_line(i):
        source = at(line[i], b)
        for n, other in enumerate(chips):
            block, sem = extra.at[n, source], extra_line_sem(n, line[i])
            arrived(CORES, sem)
            if i == 0:
                send_middle(block, sem, (dp, at(mirror, b)))
            for side in sides:
                send(block, extra_joint(n), (dp, at(a, side)))

    def extra_far():
        source = at(third, b)
        for n, other in enumerate(chips):
            for c in range(CORES):
                block = extra.at[n, source, :, pl.ds(c * feats, feats)]
                for side in [b] + sides:
                    send(block, late, (other * CORES + c, at(a, side)), cols_ref.at[chip, core, source])

    @only
    def own_last():
        arrived(n_side * (1 + n_line) * CORES + 1, own_joint)

    @only
    def extra_last():
        for n in range(n_other):
            arrived(n_side * (1 + n_line) * CORES, extra_joint(n))

    def cols_along(side):
        for other in chips:
            block = cols_ref.at[other, :, at(a, side)]
            send(block, late, (dp, at(twin, b)))
            send_middle(block, late, (dp, at(mirror, b)))
            send_middle(block, late, (dp, at(across, b)))

    @only
    def cols_own():
        arrived(n_other * CORES, cross)
        for other in chips:
            for side in sides:
                send(cols_ref.at[other, :, t], from_sides, (dp, at(a, side)))
        if has_line:
            cols_along(b)

    @only
    def cols_sides():
        if n_side:
            arrived(n_other * n_side * CORES, from_sides)
        if has_line:
            for side in sides:
                cols_along(side)

    def cols_last():
        if has_line:
            arrived(3 * n_other * (1 + n_side) * CORES, late)

    @only
    def hidden_piece(k):
        start, width = pieces[k]
        for other in chips:
            piece = hidden_ref.at[other, core, :, pl.ds(start, width)]
            copy_to(piece, hidden_sem.at[k], (mate, t), lane=1).wait_recv()
        for other in chips:
            piece = hidden_ref.at[other, core, :, pl.ds(start, width)]
            copy_to(piece, hidden_mate, (mate, t), lane=1).start()

    def scoped(name, job, *args):
        with jax.named_scope(name):
            return job(*args)

    def dot(k):
        if k >= len(spans):
            return
        if k == 0:
            for place, owner in enumerate((core, 1 - core)):
                left[pl.ds(place * group, group)] = (
                    cols_ref[chip, owner].astype(jnp.float32).reshape(group, feats).astype(jnp.bfloat16)
                )
        start, width = spans[k]
        span = pl.ds(start, width)
        term = lax.dot_general(
            left[...], weight[:, span], (((1,), (0,)), ((), ())), preferred_element_type=jnp.float32
        )
        grad_ref[:, span] = term[:group]
        leave[:, span] = term[group:].astype(jnp.bfloat16)
        copy_to(leave.at[:, span], grad_mate, (mate, t), other_ref.at[:, span], 1).start()

    def turn(q):
        for k, (raw, turned, _, start, width) in enumerate(slices):
            far = len(slices) - n_own
            if (k * TURNS // far if k < far else TURNS) == q:
                weight_loads[k].wait()
                span = pl.ds(start, width)
                turned[span] = raw[:, span].T

    jobs = {
        "own": own_line, "extra": extra_line, "cols": cols_own, "sides": cols_sides,
        "owns": own_last, "extras": extra_last, "hidden": hidden_piece, "dots": dot, "turn": turn, "far": extra_far,
    }
    line_jobs = ("own", "extra", "far")
    for name, *rest in ORDER:
        if name in line_jobs and not has_line or name == "hidden" and rest[0] >= len(pieces):
            continue
        where = rest.pop() if rest and rest[-1] in (MIDDLE, END) else None
        if where is None:
            scoped(name + "".join(map(str, rest)), jobs[name], *rest)
        else:
            scoped(name + "".join(map(str, rest)) + where[0], functools.partial(jobs[name], where=int(where == MIDDLE)), *rest)

    with jax.named_scope("tail_cols"):
        cols_last()
    with jax.named_scope("tail_hid"):
        everyone = hidden_ref.at[:, 1 - core]
        copy_to(everyone, hidden_mate, (mate, t), lane=1).wait_recv()
    with jax.named_scope("tail_grad"):
        copy_to(leave, grad_mate, (mate, t), other_ref, 1).wait_recv()
    with jax.named_scope("tail_send"):
        copy_to(gauge.at[pl.ds(0, sum(sent))], late, (mate, t)).wait_send()
        if has_line:

            @pl.when(middle == 1)
            def _():
                copy_to(gauge.at[pl.ds(0, sum(sent_middle))], late, (mate, t)).wait_send()

            @pl.when(middle == 0)
            def _():
                copy_to(gauge.at[pl.ds(0, sum(sent_end))], late, (mate, t)).wait_send()

        copy_to(hidden_ref, hidden_mate, (mate, t), lane=1).wait_send()


def finish_kernel(
    spans, chunks, cols_ref, hidden_ref, grad_ref, other_ref, act_ref, slope_ref, extra_ref, distant_ref,
    weight_out, gate_out, up_out, turned, gate, upper, left, weight_sem, grad_sem,
):
    copies = []

    def leave(src, dst, sem):
        copies.append(pltpu.make_async_copy(src, dst, sem))
        copies[-1].start()

    for k, (start, width) in enumerate(spans):
        span = pl.ds(start, width)
        turned[span] = lax.dot_general(
            hidden_ref[:, span], cols_ref[...], (((0,), (0,)), ((), ())), preferred_element_type=jnp.float32
        )
        leave(turned.at[span], weight_out.at[span], weight_sem.at[k])
    n_other, _, _, pair = extra_ref.shape
    for n in range(n_other):
        left[n] = extra_ref[n].astype(jnp.float32).reshape(left.shape[1], pair).astype(jnp.bfloat16)
    for k, (start, width) in enumerate(chunks):
        span = pl.ds(start, width)
        grad = grad_ref[:, span] + other_ref[:, span].astype(jnp.float32)
        for n in range(n_other):
            grad += jnp.dot(left[n], distant_ref[n, :, span], preferred_element_type=jnp.float32)
        upper[:, span] = (grad * act_ref[:, span]).astype(jnp.bfloat16)
        gate[:, span] = (grad * slope_ref[:, span]).astype(jnp.bfloat16)
    leave(upper, up_out, grad_sem.at[0])
    leave(gate, gate_out, grad_sem.at[1])
    for copy in copies:
        copy.wait()


def body(n_dp, n_t, grad_out, gate_pre, up_pre, down_weight):
    depth, model = grad_out.shape
    group, wide = gate_pre.shape
    feats = model // n_dp
    n_chip = n_dp // CORES
    outer = 4 if n_t % 4 == 0 else 1
    inner = n_t // outer
    spans = cut(wide, 1024)
    pieces = cut(wide, 1024)
    n_side, n_other = inner - 1, n_chip - 1
    n_gauge = (n_chip + 1) * (n_side + 4) * 2 + 3 * n_side * 2 + n_other * (16 * n_side + 12)
    lanes = pl.cdiv(wide, 128) * 128
    pair = CORES * feats
    results = 2 * (n_dp * group * (feats + lanes) + 7 * group * lanes + n_other * (group + lanes) * pair)
    limit = VMEM - results - 64 * 1024
    anywhere = pl.BlockSpec(memory_space=pltpu.HBM)
    vmem = pl.BlockSpec(memory_space=pltpu.VMEM)
    dma = pltpu.SemaphoreType.DMA
    cols, hidden, *factors = pl.pallas_call(
        functools.partial(gather_kernel, n_dp, n_t, outer, spans, pieces),
        out_shape=[
            pltpu.VMEM((n_chip, CORES, n_t, depth, feats), jnp.bfloat16),
            pltpu.VMEM((n_chip, CORES, group, wide), jnp.bfloat16),
            pltpu.VMEM((group, wide), jnp.float32),
            pltpu.VMEM((group, wide), jnp.bfloat16),
            pltpu.VMEM((group, wide), jnp.float32),
            pltpu.VMEM((group, wide), jnp.float32),
            pltpu.VMEM((n_other, n_t, depth, pair), jnp.bfloat16),
            pltpu.VMEM((n_other, pair, wide), jnp.bfloat16),
        ],
        in_specs=[anywhere] * 4,
        out_specs=[vmem] * 8,
        scratch_shapes=[
            pltpu.VMEM((depth, model), jnp.bfloat16),
            pltpu.VMEM((group, wide), jnp.bfloat16),
            pltpu.VMEM((group, wide), jnp.bfloat16),
            pltpu.VMEM((feats, wide), jnp.bfloat16),
            pltpu.VMEM((wide, feats), jnp.bfloat16),
            pltpu.VMEM((n_other, wide, pair), jnp.bfloat16),
            pltpu.VMEM((CORES * group, feats), jnp.bfloat16),
            pltpu.VMEM((group, wide), jnp.bfloat16),
            pltpu.VMEM((n_gauge, depth, feats), jnp.bfloat16),
            dma((3,)),
            dma((n_other * len(cut(pair, SLICE)) + len(cut(feats, SLICE)),)),
            dma((2,)),
            pltpu.SemaphoreType.REGULAR((2,)),
            dma((outer + 1,)),
            dma((n_other, outer + 1)),
            dma((3,)),
            dma((len(pieces) + 2,)),
        ],
        compiler_params=pltpu.CompilerParams(collective_id=0, has_side_effects=True, vmem_limit_bytes=limit),
    )(grad_out, gate_pre, up_pre, down_weight.T)
    cols = cols.reshape(n_dp * group, feats)
    hidden = hidden.reshape(n_dp * group, wide)

    steps = [(0, min(128, wide))] + [(128 + start, width) for start, width in cut(wide - 128, 256)]
    turned, grad_gate, grad_up = pl.pallas_call(
        functools.partial(finish_kernel, steps, cut(wide, 512)),
        out_shape=[
            jax.ShapeDtypeStruct((wide, feats), jnp.float32),
            jax.ShapeDtypeStruct((group, wide), jnp.bfloat16),
            jax.ShapeDtypeStruct((group, wide), jnp.bfloat16),
        ],
        in_specs=[vmem] * 8,
        out_specs=[anywhere] * 3,
        scratch_shapes=[
            pltpu.VMEM((wide, feats), jnp.float32),
            pltpu.VMEM((group, wide), jnp.bfloat16),
            pltpu.VMEM((group, wide), jnp.bfloat16),
            pltpu.VMEM((n_other, group, pair), jnp.bfloat16),
            dma((len(steps),)),
            dma((2,)),
        ],
        compiler_params=pltpu.CompilerParams(vmem_limit_bytes=limit),
    )(*[pltpu.with_memory_space_constraint(x, pltpu.VMEM) for x in (cols, hidden, *factors)])
    return turned.T, grad_gate, grad_up


def solution(mesh):
    in_specs = (P(("dp", "tensor"), None), P("dp", "tensor"), P("dp", "tensor"), P(None, "tensor"))
    out_specs = (P("dp", "tensor"), P("dp", "tensor"), P("dp", "tensor"))
    fn = functools.partial(body, mesh.shape["dp"], mesh.shape["tensor"])
    return jax.shard_map(fn, mesh=mesh, in_specs=in_specs, out_specs=out_specs, check_vma=False)
```
